64 devices in a mesh: dp: 4 (over x, y), ep: 16 (over z, core).
Axes of the slice: x: 2, y: 2, z: 8, core: 2. Of those that a mesh axis runs over, the one named last changes fastest.
The devices are a block of a 4x4x8 slice.
Arguments:
- x_tok: bfloat16 [4096, 2560], P(('dp', 'ep')), parts along dimension 0
- topk_idx: int32 [4096, 6], P(('dp', 'ep')), parts along dimension 0
- topk_w: float32 [4096, 6], P(('dp', 'ep')), parts along dimension 0
- w_in: bfloat16 [64, 2560, 1536], P('ep')
- w_out: bfloat16 [64, 1536, 2560], P('ep')
- shared_in: bfloat16 [2560, 3072], replicated
- shared_out: bfloat16 [3072, 2560], replicated
Outputs:
- output: bfloat16 [4096, 2560], P(('dp', 'ep')), parts along dimension 0
There are 4 independent parts. The reference program is written for one: setup_inputs(seed, part) draws one part's arguments, and reference() takes and returns one part's arrays. A program takes and returns all parts, laid end to end along the dimension named above; an argument that names none is the same for every part.
All inputs are finite; a program needn't handle non-finite values.
Results may differ from the reference program's by a relative error of at most 0.001.
Values are sent between devices in bfloat16 or wider.
A program may use at most 768 MiB of HBM per device.

```python
import jax
import jax.numpy as jnp
from jax import lax

GROUP_SIZE = 16
TOK_DEV = 64
D_MODEL = 2560
FF_DIM = 1536
FS_DIM = 3072
EXPERTS = 64
TOP_K = 6
NUM_HOT = 2
SLOT_CAP = 18

TOKENS = GROUP_SIZE * TOK_DEV
EXPERT_ROWS = SLOT_CAP * GROUP_SIZE


def draw_routing(route_key):
    key_hot, key_extra, key_tok, key_rot = jax.random.split(route_key, 4)
    cold_count = EXPERTS - NUM_HOT
    rest_pairs = TOK_DEV * TOP_K - NUM_HOT * SLOT_CAP
    base_load = rest_pairs // cold_count
    extra_pairs = rest_pairs - base_load * cold_count
    expert_order = jax.random.permutation(key_hot, EXPERTS)
    cold_rank = jax.vmap(lambda dev_key: jax.random.permutation(dev_key, cold_count))(jax.random.split(key_extra, GROUP_SIZE))
    cold_load = base_load + (cold_rank < extra_pairs).astype(jnp.int32)
    hot_load = jnp.full((GROUP_SIZE, NUM_HOT), SLOT_CAP, jnp.int32)
    ordered_load = jnp.concatenate([hot_load, cold_load], axis=1)
    expert_load = jnp.zeros((GROUP_SIZE, EXPERTS), jnp.int32).at[:, expert_order].set(ordered_load)
    load_ends = jnp.cumsum(expert_load, axis=1)
    pair_ids = jnp.arange(TOK_DEV * TOP_K, dtype=jnp.int32)
    pair_expert = jax.vmap(lambda ends_row: jnp.searchsorted(ends_row, pair_ids, side='right'))(load_ends)
    slot_table = pair_expert.reshape(GROUP_SIZE, TOP_K, TOK_DEV).transpose(0, 2, 1)
    tok_perm = jax.vmap(lambda dev_key: jax.random.permutation(dev_key, TOK_DEV))(jax.random.split(key_tok, GROUP_SIZE))
    tok_index = jnp.broadcast_to(tok_perm[:, :, None], (GROUP_SIZE, TOK_DEV, TOP_K))
    slot_table = jnp.take_along_axis(slot_table, tok_index, axis=1)
    slot_shift = jax.random.randint(key_rot, (GROUP_SIZE, TOK_DEV, 1), 0, TOP_K)
    slot_cols = (jnp.arange(TOP_K)[None, None, :] + slot_shift) % TOP_K
    slot_table = jnp.take_along_axis(slot_table, slot_cols, axis=2)
    return slot_table.reshape(TOKENS, TOP_K).astype(jnp.int32)


def draw_stack(stack_key, fan_in, fan_out):
    def one_expert(expert_key):
        return (jax.random.normal(expert_key, (fan_in, fan_out), jnp.float32) * fan_in ** -0.5).astype(jnp.bfloat16)
    return lax.map(one_expert, jax.random.split(stack_key, EXPERTS))


def setup_inputs(seed: int = 0, part: int = 0) -> dict:
    root_key = jax.random.key(seed)
    key_x, key_route, key_gate, key_in, key_out, key_sin, key_sout = jax.random.split(root_key, 7)
    x_tok = jax.random.normal(jax.random.fold_in(key_x, part), (TOKENS, D_MODEL), jnp.float32).astype(jnp.bfloat16)
    topk_idx = draw_routing(jax.random.fold_in(key_route, part))
    gate_raw = jax.random.uniform(jax.random.fold_in(key_gate, part), (TOKENS, TOP_K), jnp.float32, 0.2, 1.0)
    topk_w = gate_raw * (1.5 / TOP_K ** 0.5)
    w_in = draw_stack(key_in, D_MODEL, FF_DIM)
    w_out = draw_stack(key_out, FF_DIM, D_MODEL)
    shared_in = (jax.random.normal(key_sin, (D_MODEL, FS_DIM), jnp.float32) * D_MODEL ** -0.5).astype(jnp.bfloat16)
    shared_out = (jax.random.normal(key_sout, (FS_DIM, D_MODEL), jnp.float32) * FS_DIM ** -0.5).astype(jnp.bfloat16)
    return {'x_tok': x_tok, 'topk_idx': topk_idx, 'topk_w': topk_w, 'w_in': w_in, 'w_out': w_out, 'shared_in': shared_in, 'shared_out': shared_out}


def reference(x_tok, topk_idx, topk_w, w_in, w_out, shared_in, shared_out):
    pair_total = TOKENS * TOP_K
    flat_ids = topk_idx.reshape(pair_total)
    pair_order = jnp.argsort(flat_ids, stable=True)
    counts = jnp.zeros((EXPERTS,), jnp.int32).at[flat_ids].add(1)
    starts = jnp.cumsum(counts) - counts
    pair_gates = topk_w.astype(jnp.bfloat16).astype(jnp.float32).reshape(pair_total)
    slot_ids = jnp.arange(EXPERT_ROWS)

    def expert_step(routed_acc, step_in):
        e_index, w_first, w_second = step_in
        slot_valid = slot_ids < counts[e_index]
        pair_pos = pair_order[jnp.minimum(starts[e_index] + slot_ids, pair_total - 1)]
        tok_pos = pair_pos // TOP_K
        gathered = x_tok[tok_pos]
        hidden = jax.nn.gelu(jnp.dot(gathered, w_first, preferred_element_type=jnp.float32), approximate=True).astype(jnp.bfloat16)
        expert_out = jnp.dot(hidden, w_second, preferred_element_type=jnp.float32).astype(jnp.bfloat16)
        pair_scale = jnp.where(slot_valid, pair_gates[pair_pos], 0.0)
        contrib = expert_out.astype(jnp.float32) * pair_scale[:, None]
        return routed_acc.at[tok_pos].add(contrib), None

    routed_init = jnp.zeros((TOKENS, D_MODEL), jnp.float32)
    routed, _ = lax.scan(expert_step, routed_init, (jnp.arange(EXPERTS), w_in, w_out))
    shared_hidden = jax.nn.gelu(jnp.dot(x_tok, shared_in, preferred_element_type=jnp.float32), approximate=True).astype(jnp.bfloat16)
    shared_val = jnp.dot(shared_hidden, shared_out, preferred_element_type=jnp.float32)
    return (routed + shared_val).astype(jnp.bfloat16)
```

```python
import jax
import jax.numpy as jnp
from jax import lax
from jax.sharding import PartitionSpec as P

LOAD_MULT = 3


def solution(mesh):
    group_size = mesh.shape['ep']

    def local_layer(x_loc, idx_loc, gate_loc, w_in, w_out, shared_in, shared_out):
        tok_rows, top_k = idx_loc.shape
        own_experts = w_in.shape[0]
        num_experts = own_experts * group_size
        slot_cap = min(tok_rows, LOAD_MULT * tok_rows * top_k // num_experts)
        x_all = lax.all_gather(x_loc, 'ep', axis=0, tiled=True)
        picks = (idx_loc[:, :, None] == jnp.arange(num_experts, dtype=jnp.int32))
        picked = jnp.any(picks, axis=1)
        rank = jnp.cumsum(picked.astype(jnp.int32), axis=0) - 1
        gates = jnp.sum(jnp.where(picks, gate_loc.astype(jnp.bfloat16).astype(jnp.float32)[:, :, None], 0.0), axis=1)
        code = jnp.where(picked, rank, -1).astype(jnp.float32)
        table = jnp.stack([code, gates], axis=0).reshape(2, tok_rows, group_size, own_experts)
        table = lax.all_to_all(table, 'ep', 2, 1, tiled=True)
        table = table.reshape(2, group_size, tok_rows, own_experts)
        code_all, gate_all = table[0], table[1]
        hot = (code_all[:, :, :, None] == jnp.arange(slot_cap, dtype=jnp.float32))
        own = jnp.eye(group_size, dtype=jnp.bool_)
        disp = (hot[:, :, :, None, :] & own[:, None, None, :, None])
        combine = jnp.where(disp, gate_all[:, :, :, None, None], 0.0).astype(jnp.bfloat16)
        rows = group_size * slot_cap
        disp = disp.astype(jnp.bfloat16).reshape(group_size * tok_rows, own_experts, rows)
        combine = combine.reshape(group_size * tok_rows, own_experts, rows)
        recv_rows = jnp.einsum('ter,tm->erm', disp, x_all, preferred_element_type=jnp.float32).astype(jnp.bfloat16)
        hidden = jax.nn.gelu(jnp.einsum('erm,emf->erf', recv_rows, w_in, preferred_element_type=jnp.float32), approximate=True).astype(jnp.bfloat16)
        expert_out = jnp.einsum('erf,efm->erm', hidden, w_out, preferred_element_type=jnp.float32).astype(jnp.bfloat16)
        partial = jnp.einsum('ter,erm->tm', combine, expert_out, preferred_element_type=jnp.float32)
        routed = lax.psum_scatter(partial, 'ep', scatter_dimension=0, tiled=True)
        shared_hidden = jax.nn.gelu(jnp.dot(x_loc, shared_in, preferred_element_type=jnp.float32), approximate=True).astype(jnp.bfloat16)
        shared_val = jnp.dot(shared_hidden, shared_out, preferred_element_type=jnp.float32)
        return (routed + shared_val).astype(jnp.bfloat16)

    tok_spec = P(('dp', 'ep'), None)
    expert_spec = P('ep', None, None)
    whole_spec = P(None, None)
    return jax.shard_map(local_layer, mesh=mesh, in_specs=(tok_spec, tok_spec, tok_spec, expert_spec, expert_spec, whole_spec, whole_spec), out_specs=tok_spec, check_vma=False)
```

```python
import functools

import jax
import jax.numpy as jnp
from jax import lax
from jax.experimental import pallas as pl
from jax.experimental.pallas import tpu as pltpu
from jax.sharding import PartitionSpec as P

LOAD_MULT = 3
COLS = 256
LEAD = 3
CORES = 2
ABSENT = -4096.0
VMEM_BYTES = 67_000_000
F32 = jnp.float32
BF16 = jnp.bfloat16


def gelu(z):
    return 0.5 * z * (1.0 + jnp.tanh(0.7978845608028654 * (z + 0.044715 * (z * z * z))))


def moe_kernel(chips, cap, top_k,
               x_hbm, tab_hbm, wi_hbm, wo_hbm, si_hbm, so_hbm, y_ref,
               x_all, tabs, picks, codes, pick_mat, gate_mat, xg, hacc, h, outs, pbuf, ppush, prec, rbuf,
               sacc, s_act, u_all, wi_buf, wo_buf, si_buf, so_buf,
               ag_recv, tab_recv, ag_part, tab_part, ag_send, tab_send, own_sem,
               rs_recv, rs_send, pp_send, pp_recv, wi_sem, wo_sem, si_sem, so_sem):
    rows, d_model = x_hbm.shape
    experts = wi_hbm.shape[0]
    nc = d_model // COLS
    hops = chips // 2
    half = rows // 2
    group_rows = chips * rows
    slots = chips * cap

    ep = lax.axis_index('ep')
    z, c = ep // CORES, ep % CORES
    partner = {'ep': z * CORES + (1 - c)}
    nxt = {'ep': ((z + 1) % chips) * CORES + c}
    prv = {'ep': ((z + chips - 1) % chips) * CORES + c}

    def chip(off):
        return (z + off + chips) % chips

    def xrows(w, s, lo=0, count=None):
        base = (c * chips + s) * rows + lo
        return x_all.at[w, pl.ds(pl.multiple_of(base, half), rows if count is None else count)]

    def tblk(s, lo=0, count=None):
        t = tabs.at[c * chips + s]
        return t if count is None else t.at[pl.ds(lo, count)]

    def remote(src, dst, ssem, rsem, dev):
        return pltpu.make_async_remote_copy(src_ref=src, dst_ref=dst, send_sem=ssem, recv_sem=rsem, device_id=dev, device_id_type=pl.DeviceIdType.MESH)

    def ag_copy(w, k, up):
        s = chip(-(k - 1)) if up else chip(k - 1)
        lo, cnt = (0, None) if k < hops else ((0, half) if up else (half, half))
        ref = xrows(w, s, lo, cnt)
        return remote(ref, ref, ag_send.at[w], ag_recv.at[0 if up else 1, w, k - 1], nxt if up else prv)

    def ag_arrival(w, k, up):
        s = chip(-k) if up else chip(k)
        lo, cnt = (0, None) if k < hops else ((0, half) if up else (half, half))
        ref = xrows(w, s, lo, cnt)
        return remote(ref, ref, ag_send.at[w], ag_recv.at[0 if up else 1, w, k - 1], nxt if up else prv)

    def tab_copy(k, up, arrival):
        off = k if arrival else k - 1
        s = chip(-off) if up else chip(off)
        lo, cnt = (0, None) if k < hops else ((0, 8) if up else (8, 8))
        ref = tblk(s, lo, cnt)
        return remote(ref, ref, tab_send, tab_recv.at[0 if up else 1, k - 1], nxt if up else prv)

    def ag_push(w, s):
        ref = xrows(w, s)
        return remote(ref, ref, ag_send.at[w], ag_part.at[w], partner)

    def tab_push(s):
        ref = tblk(s)
        return remote(ref, ref, tab_send, tab_part, partner)

    def wi_copy(w):
        return pltpu.make_async_copy(wi_hbm.at[:, pl.ds(pl.multiple_of(w * COLS, COLS), COLS), :], wi_buf.at[w % 2], wi_sem.at[w % 2])

    def wo_copy(w):
        return pltpu.make_async_copy(wo_hbm.at[:, :, pl.ds(pl.multiple_of(w * COLS, COLS), COLS)], wo_buf.at[w % 2], wo_sem.at[w % 2])

    def si_copy(w):
        return pltpu.make_async_copy(si_hbm.at[pl.ds(pl.multiple_of(w * COLS, COLS), COLS), :], si_buf.at[w % 2], si_sem.at[w % 2])

    def so_copy(w):
        return pltpu.make_async_copy(so_hbm.at[:, pl.ds(pl.multiple_of(w * COLS, COLS), COLS)], so_buf.at[w % 2], so_sem.at[w % 2])

    for w in range(nc):
        pltpu.make_async_copy(x_hbm.at[:, pl.ds(w * COLS, COLS)], xrows(w, z), own_sem.at[0]).start()
    pltpu.make_async_copy(tab_hbm, tblk(z), own_sem.at[1]).start()
    for w in range(2):
        si_copy(w).start()
    for w in range(2):
        wi_copy(w).start()

    barrier = pltpu.get_barrier_semaphore()
    for dev in (nxt, prv, partner):
        pl.semaphore_signal(barrier, inc=1, device_id=dev, device_id_type=pl.DeviceIdType.MESH)
    pl.semaphore_wait(barrier, 3)

    pltpu.make_async_copy(tab_hbm, tblk(z), own_sem.at[1]).wait()
    own_all = x_all.at[0, pl.ds(0, nc * rows)]
    pltpu.make_async_copy(own_all, own_all, own_sem.at[0]).wait()
    tab_copy(1, True, False).start()
    tab_copy(1, False, False).start()
    tab_push(z).start()
    for w in range(min(LEAD, nc)):
        ag_copy(w, 1, True).start()
        ag_copy(w, 1, False).start()
        ag_push(w, z).start()
    for w in range(2):
        wo_copy(w).start()
        so_copy(w).start()

    def build_tables():
        base = (ep * experts).astype(F32)
        lane = lax.broadcasted_iota(jnp.int32, (1, 2 * rows), 1)
        pairs = chips // 2
        for g in range(2):
            cc = c if g == 0 else 1 - c
            for i in range(pairs):
                t = tabs[cc * chips + 2 * i] + tabs[cc * chips + 2 * i + 1]
                ids, gts = t[0:top_k], t[8:8 + top_k]
                for e in range(experts):
                    hit = ids == (base + float(e))
                    r = (g * pairs + i) * experts + e
                    picks[r:r + 1, :] = jnp.sum(hit.astype(F32), axis=0, keepdims=True)
                    codes[g, experts + e:experts + e + 1, i * 2 * rows:(i + 1) * 2 * rows] = jnp.sum(jnp.where(hit, gts, 0.0), axis=0, keepdims=True)
        a = lax.broadcasted_iota(jnp.int32, (2 * rows, 2 * rows), 0)
        b = lax.broadcasted_iota(jnp.int32, (2 * rows, 2 * rows), 1)
        before = ((a < b) & ((a >= rows) == (b >= rows))).astype(F32).astype(BF16)
        rank = jnp.dot(picks[...].astype(BF16), before, preferred_element_type=F32)
        for g in range(2):
            for i in range(pairs):
                start = (2 * i * cap + jnp.where(lane >= rows, cap, 0)).astype(F32)
                for e in range(experts):
                    r = (g * pairs + i) * experts + e
                    code = jnp.where(picks[r:r + 1, :] > 0.5, rank[r:r + 1, :] + start, ABSENT)
                    codes[g, e:e + 1, i * 2 * rows:(i + 1) * 2 * rows] = code
        slot = lax.broadcasted_iota(jnp.int32, (slots, group_rows), 0).astype(F32)
        col = lax.broadcasted_iota(jnp.int32, (2 * rows, experts * slots), 1).astype(F32)
        for g in range(2):
            for e in range(experts):
                pick_mat[g, e * slots:(e + 1) * slots, :] = jnp.where(slot == codes[g, e:e + 1, :], 1.0, 0.0).astype(BF16)
            for i in range(pairs):
                ct = jnp.transpose(codes[g, :, i * 2 * rows:(i + 1) * 2 * rows])
                acc = jnp.zeros((2 * rows, experts * slots), F32)
                for e in range(experts):
                    acc = jnp.where(col == ct[:, e:e + 1] + float(e * slots), ct[:, experts + e:experts + e + 1], acc)
                gate_mat[g, i * 2 * rows:(i + 1) * 2 * rows, :] = acc.astype(BF16)

    def gather(w, g):
        cc = c if g == 0 else 1 - c
        xs = x_all[w, pl.ds(pl.multiple_of(cc * group_rows, group_rows), group_rows), :]
        got = jnp.dot(pick_mat[g], xs, preferred_element_type=F32).astype(BF16)
        for e in range(experts):
            xg[e, g * slots:(g + 1) * slots, :] = got[e * slots:(e + 1) * slots, :]

    def in_step(j, carry):
        w = j + LEAD

        @pl.when(w < nc)
        def _():
            ag_copy(w, 1, True).start()
            ag_copy(w, 1, False).start()
            ag_push(w, z).start()

        for k in range(1, hops):
            w = j - (k - 1)

            @pl.when((w >= 0) & (w < nc))
            def _():
                if k >= 1:
                    @pl.when(w == 0)
                    def _():
                        for up in (True, False):
                            tab_copy(k, up, True).wait_recv()
                            tab_copy(k + 1, up, False).start()
                        tab_push(chip(-k)).start()
                        tab_push(chip(k)).start()
                for up in (True, False):
                    ag_arrival(w, k, up).wait_recv()
                    ag_copy(w, k + 1, up).start()
                ag_push(w, chip(-k)).start()
                ag_push(w, chip(k)).start()

        w = j - (hops - 1)

        @pl.when((w >= 0) & (w < nc))
        def _():
            for up in (True, False):
                ag_arrival(w, hops, up).wait_recv()
            ag_push(w, chip(hops)).start()

            @pl.when(w == 0)
            def _():
                for up in (True, False):
                    tab_copy(hops, up, True).wait_recv()
                tab_push(chip(hops)).start()

        @pl.when(j < nc)
        def _():
            si_copy(j).wait()
            mine = x_all[j, pl.ds(pl.multiple_of((c * chips + z) * rows, rows), rows), :]
            part = jnp.dot(mine, si_buf[j % 2], preferred_element_type=F32)

            @pl.when(j == 0)
            def _():
                sacc[...] = part

            @pl.when(j > 0)
            def _():
                sacc[...] += part

            @pl.when(j + 2 < nc)
            def _():
                si_copy(j + 2).start()

        @pl.when((w >= 0) & (w < nc))
        def _():
            @pl.when(w == 0)
            def _():
                theirs = tabs.at[pl.ds((1 - c) * chips, chips)]
                pltpu.make_async_copy(theirs, theirs, tab_part).wait()
                build_tables()

            gather(w, 0)
            theirs = x_all.at[w, pl.ds(pl.multiple_of((1 - c) * group_rows, group_rows), group_rows)]
            pltpu.make_async_copy(theirs, theirs, ag_part.at[w]).wait()
            gather(w, 1)
            wi_copy(w).wait()

            @pl.when(w == 0)
            def _():
                hacc[...] = jnp.zeros_like(hacc)

            for e in range(experts):
                hacc[e] += jnp.dot(xg[e], wi_buf[w % 2, e], preferred_element_type=F32)

            @pl.when(w + 2 < nc)
            def _():
                wi_copy(w + 2).start()

        return carry

    lax.fori_loop(0, nc + hops - 1, in_step, 0)

    def act_step(e, carry):
        h[e] = gelu(hacc[e]).astype(BF16)
        return carry

    lax.fori_loop(0, experts, act_step, 0)
    s_act[...] = gelu(sacc[...]).astype(BF16)

    def prow(w, s, lo=0, count=None):
        return pbuf.at[w, pl.ds(pl.multiple_of(s * rows + lo, half), rows if count is None else count)]

    def rs_copy(w, k, up):
        off = hops - k + 1
        s = chip(off) if up else chip(-off)
        lo, cnt = (0, rows) if k > 1 else ((0, half) if up else (half, half))
        d = 0 if up else 1
        return remote(prow(w, s, lo, cnt), rbuf.at[d, w, k - 1, pl.ds(lo, cnt)], rs_send.at[w], rs_recv.at[d, w, k - 1], nxt if up else prv)

    def push_copy(w):
        return remote(ppush.at[w % 2], prec.at[w % 2], pp_send.at[w % 2], pp_recv.at[w % 2], partner)

    def out_step(i, carry):
        @pl.when(i < nc)
        def _():
            wo_copy(i).wait()
            for e in range(experts):
                o = jnp.dot(h[e], wo_buf[i % 2, e], preferred_element_type=F32).astype(BF16)
                outs[0, e * slots:(e + 1) * slots, :] = o[:slots]
                outs[1, e * slots:(e + 1) * slots, :] = o[slots:]

            @pl.when(i >= 2)
            def _():
                push_copy(i).wait_send()

            ppush[i % 2] = jnp.dot(gate_mat[1], outs[1], preferred_element_type=F32)
            push_copy(i).start()
            pbuf[i] = jnp.dot(gate_mat[0], outs[0], preferred_element_type=F32)
            so_copy(i).wait()
            u_all[i] = jnp.dot(s_act[...], so_buf[i % 2], preferred_element_type=F32)

            @pl.when(i + 2 < nc)
            def _():
                wo_copy(i + 2).start()
                so_copy(i + 2).start()

            push_copy(i).wait_recv()
            pbuf[i] += prec[i % 2]
            rs_copy(i, 1, True).start()
            rs_copy(i, 1, False).start()

        for k in range(hops - 1, 0, -1):
            w = i - k

            @pl.when((w >= 0) & (w < nc))
            def _():
                for up in (True, False):
                    rs_copy(w, k, up).wait_recv()
                    d = 0 if up else 1
                    s = chip(hops - k) if up else chip(-(hops - k))
                    lo, cnt = (0, rows) if k > 1 else ((0, half) if up else (half, half))
                    dst = prow(w, s, lo, cnt)
                    dst[...] += rbuf[d, w, k - 1, lo:lo + cnt, :]
                    rs_copy(w, k + 1, up).start()

        w = i - hops

        @pl.when(w >= 0)
        def _():
            rs_copy(w, hops, True).wait_recv()
            rs_copy(w, hops, False).wait_recv()
            total = prow(w, z)[...] + (rbuf[0, w, hops - 1] + rbuf[1, w, hops - 1]) + u_all[w]
            y_ref[:, pl.ds(pl.multiple_of(w * COLS, COLS), COLS)] = total.astype(BF16)

        return carry

    lax.fori_loop(0, nc + hops, out_step, 0)

    def drain(w, carry):
        sent = x_all.at[w, pl.ds(0, (2 * chips - 1) * rows)]
        pltpu.make_async_copy(sent, sent, ag_send.at[w]).wait()
        sums = pbuf.at[w, pl.ds(0, (chips - 1) * rows)]
        pltpu.make_async_copy(sums, sums, rs_send.at[w]).wait()
        return carry

    lax.fori_loop(0, nc, drain, 0)
    sent = tabs.at[pl.ds(0, 2 * chips - 1)]
    pltpu.make_async_copy(sent, sent, tab_send).wait()
    for w in range(min(2, nc)):
        push_copy(w).wait_send()


def solution(mesh):
    group_size = mesh.shape['ep']
    chips = group_size // CORES
    hops = chips // 2

    def local_layer(x_loc, idx_loc, gate_loc, w_in, w_out, shared_in, shared_out):
        rows, top_k = idx_loc.shape
        d_model = x_loc.shape[1]
        experts, _, ff = w_in.shape
        fs = shared_in.shape[1]
        num_experts = experts * group_size
        cap = min(rows, LOAD_MULT * rows * top_k // num_experts)
        slots = chips * cap
        nc = d_model // COLS
        parity = (lax.axis_index('ep') // CORES) % 2
        pad = jnp.zeros((8 - top_k, rows), F32)
        tab = jnp.concatenate([idx_loc.T.astype(F32), pad, gate_loc.T, pad], axis=0)
        side = (jnp.arange(2 * rows)[None, :] >= rows) == (parity == 1)
        tab = jnp.where(side, jnp.concatenate([tab, tab], axis=1), 0.0)
        any_spec = pl.BlockSpec(memory_space=pl.ANY)
        dma = pltpu.SemaphoreType.DMA
        flops = 2 * group_size * cap * experts * d_model * ff * 2
        return pl.pallas_call(
            functools.partial(moe_kernel, chips, cap, top_k),
            out_shape=jax.ShapeDtypeStruct((rows, d_model), BF16),
            in_specs=[any_spec] * 6,
            out_specs=pl.BlockSpec(memory_space=pltpu.VMEM),
            scratch_shapes=[
                pltpu.VMEM((nc, group_size * rows, COLS), BF16),
                pltpu.VMEM((group_size, 16, 2 * rows), F32),
                pltpu.VMEM((chips * experts, 2 * rows), F32),
                pltpu.VMEM((2, 2 * experts, chips * rows), F32),
                pltpu.VMEM((2, experts * slots, chips * rows), BF16),
                pltpu.VMEM((2, chips * rows, experts * slots), BF16),
                pltpu.VMEM((experts, 2 * slots, COLS), BF16),
                pltpu.VMEM((experts, 2 * slots, ff), F32),
                pltpu.VMEM((experts, 2 * slots, ff), BF16),
                pltpu.VMEM((2, experts * slots, COLS), BF16),
                pltpu.VMEM((nc, chips * rows, COLS), F32),
                pltpu.VMEM((2, chips * rows, COLS), F32),
                pltpu.VMEM((2, chips * rows, COLS), F32),
                pltpu.VMEM((2, nc, hops, rows, COLS), F32),
                pltpu.VMEM((rows, fs), F32),
                pltpu.VMEM((rows, fs), BF16),
                pltpu.VMEM((nc, rows, COLS), F32),
                pltpu.VMEM((2, experts, COLS, ff), BF16),
                pltpu.VMEM((2, experts, ff, COLS), BF16),
                pltpu.VMEM((2, COLS, fs), BF16),
                pltpu.VMEM((2, fs, COLS), BF16),
                dma((2, nc, hops)), dma((2, hops)), dma((nc,)), dma(()), dma((nc,)), dma(()), dma((2,)),
                dma((2, nc, hops)), dma((nc,)), dma((2,)), dma((2,)),
                dma((2,)), dma((2,)), dma((2,)), dma((2,)),
            ],
            compiler_params=pltpu.CompilerParams(collective_id=0, has_side_effects=True, vmem_limit_bytes=VMEM_BYTES),
            cost_estimate=pl.CostEstimate(flops=flops, bytes_accessed=2 * (w_in.size + w_out.size + shared_in.size + shared_out.size), transcendentals=0),
        )(x_loc, tab, w_in, w_out, shared_in, shared_out)

    tok_spec = P(('dp', 'ep'), None)
    expert_spec = P('ep', None, None)
    whole_spec = P(None, None)
    return jax.shard_map(local_layer, mesh=mesh, in_specs=(tok_spec, tok_spec, tok_spec, expert_spec, expert_spec, whole_spec, whole_spec), out_specs=tok_spec, check_vma=False)
```

```python
import functools

import jax
import jax.numpy as jnp
from jax import lax
from jax.experimental import pallas as pl
from jax.experimental.pallas import tpu as pltpu
from jax.sharding import PartitionSpec as P

LOAD_MULT = 3
COLS = 256
LEAD = 4
AG_LAG = 2
RS_LAG = 2
PAIR = 2
CORES = 2
ABSENT = -4096.0
VMEM_BYTES = 67_000_000
F32 = jnp.float32
BF16 = jnp.bfloat16


def gelu(z):
    return 0.5 * z * (1.0 + jnp.tanh(0.7978845608028654 * (z + 0.044715 * (z * z * z))))


def moe_kernel(chips, cap, top_k,
               x_hbm, idx_hbm, top_hbm, wi_hbm, wo_hbm, si_hbm, so_hbm, y_ref,
               x_all, idx_v, top_v, tabs, picks, codes, pick_mat, gate_mat, xg, hacc, h, outs, pbuf, ppush, prec, rbuf,
               sacc, s_act, u_all, wi_buf, wo_buf, si_buf, so_buf,
               ag_recv, tab_recv, ag_part, tab_part, ag_send, tab_send, own_sem,
               rs_recv, rs_send, pp_send, pp_recv, wi_sem, wo_sem, si_sem, so_sem):
    rows, d_model = x_hbm.shape
    experts = wi_hbm.shape[0]
    nc = d_model // COLS
    hops = chips // 2
    half = rows // 2
    group_rows = chips * rows
    slots = chips * cap

    ep = lax.axis_index('ep')
    z, c = ep // CORES, ep % CORES
    first = lax.axis_index('dp') * (chips * CORES)
    partner = first + z * CORES + (1 - c)
    nxt = first + ((z + 1) % chips) * CORES + c
    prv = first + ((z + chips - 1) % chips) * CORES + c
    near = [(z + off) % chips for off in range(chips)]

    def chip(off):
        return near[off % chips]

    def xrows(w, s, lo=0, count=None):
        base = (c * chips + s) * rows + lo
        return x_all.at[w, pl.ds(pl.multiple_of(base, half), rows if count is None else count)]

    def tblk(s, lo=0, count=None):
        t = tabs.at[c * chips + s]
        return t if count is None else t.at[pl.ds(lo, count)]

    def remote(src, dst, ssem, rsem, dev):
        return pltpu.make_async_remote_copy(src_ref=src, dst_ref=dst, send_sem=ssem, recv_sem=rsem, device_id=dev, device_id_type=pl.DeviceIdType.LOGICAL)

    def ag_copy(w, k, up):
        s = chip(-(k - 1)) if up else chip(k - 1)
        lo, cnt = (0, None) if k < hops else ((0, half) if up else (half, half))
        ref = xrows(w, s, lo, cnt)
        return remote(ref, ref, ag_send.at[w], ag_recv.at[0 if up else 1, w, k - 1], nxt if up else prv)

    def ag_arrival(w, k, up):
        s = chip(-k) if up else chip(k)
        lo, cnt = (0, None) if k < hops else ((0, half) if up else (half, half))
        ref = xrows(w, s, lo, cnt)
        return remote(ref, ref, ag_send.at[w], ag_recv.at[0 if up else 1, w, k - 1], nxt if up else prv)

    def tab_copy(k, up, arrival):
        off = k if arrival else k - 1
        s = chip(-off) if up else chip(off)
        lo, cnt = (0, None) if k < hops else ((0, 8) if up else (8, 8))
        ref = tblk(s, lo, cnt)
        return remote(ref, ref, tab_send, tab_recv.at[0 if up else 1, k - 1], nxt if up else prv)

    def ag_push(w, s):
        ref = xrows(w, s)
        return remote(ref, ref, ag_send.at[w], ag_part.at[w], partner)

    def tab_push(s):
        ref = tblk(s)
        return remote(ref, ref, tab_send, tab_part, partner)

    def wi_copy(w):
        return pltpu.make_async_copy(wi_hbm.at[:, pl.ds(pl.multiple_of(w * PAIR * COLS, COLS), PAIR * COLS), :], wi_buf.at[w % 2], wi_sem.at[w % 2])

    def wo_copy(w):
        return pltpu.make_async_copy(wo_hbm.at[:, :, pl.ds(pl.multiple_of(w * COLS, COLS), COLS)], wo_buf.at[w % 2], wo_sem.at[w % 2])

    def si_copy(w):
        return pltpu.make_async_copy(si_hbm.at[pl.ds(pl.multiple_of(w * COLS, COLS), COLS), :], si_buf.at[w % 2], si_sem.at[w % 2])

    def so_copy(w):
        return pltpu.make_async_copy(so_hbm.at[:, pl.ds(pl.multiple_of(w * COLS, COLS), COLS)], so_buf.at[w % 2], so_sem.at[w % 2])

    for w in range(nc):
        pltpu.make_async_copy(x_hbm.at[:, pl.ds(w * COLS, COLS)], xrows(w, z), own_sem.at[0]).start()
    pltpu.make_async_copy(idx_hbm, idx_v, own_sem.at[1]).start()
    pltpu.make_async_copy(top_hbm, top_v, own_sem.at[2]).start()
    for w in range(2):
        si_copy(w).start()
    for w in range(2):
        wi_copy(w).start()

    barrier = pltpu.get_barrier_semaphore()
    for dev in (nxt, prv, partner):
        pl.semaphore_signal(barrier, inc=1, device_id=dev, device_id_type=pl.DeviceIdType.LOGICAL)
    pl.semaphore_wait(barrier, 3)

    pltpu.make_async_copy(idx_hbm, idx_v, own_sem.at[1]).wait()
    pltpu.make_async_copy(top_hbm, top_v, own_sem.at[2]).wait()
    right = lax.broadcasted_iota(jnp.int32, (top_k, 2 * rows), 1) >= rows
    side = right == (z % 2 == 1)
    ids, gts = idx_v[...].astype(F32), top_v[...]
    mine = tabs.at[c * chips + z]
    mine[...] = jnp.zeros_like(mine)
    mine[0:top_k, :] = jnp.where(side, jnp.concatenate([ids, ids], axis=1), 0.0)
    mine[8:8 + top_k, :] = jnp.where(side, jnp.concatenate([gts, gts], axis=1), 0.0)
    own_all = x_all.at[0, pl.ds(0, nc * rows)]
    pltpu.make_async_copy(own_all, own_all, own_sem.at[0]).wait()
    for w in range(min(LEAD, nc)):
        ag_copy(w, 1, True).start()
        ag_copy(w, 1, False).start()
        if w == 0:
            tab_copy(1, True, False).start()
            tab_copy(1, False, False).start()
            tab_push(z).start()
        ag_push(w, z).start()
    for w in range(2):
        wo_copy(w).start()
        so_copy(w).start()

    hacc[...] = jnp.zeros_like(hacc)

    def build_tables():
        base = (ep * experts).astype(F32)
        lane = lax.broadcasted_iota(jnp.int32, (1, 2 * rows), 1)
        pairs = chips // 2
        for g in range(2):
            cc = c if g == 0 else 1 - c
            for i in range(pairs):
                t = tabs[cc * chips + 2 * i] + tabs[cc * chips + 2 * i + 1]
                ids, gts = t[0:top_k], t[8:8 + top_k]
                for e in range(experts):
                    hit = ids == (base + float(e))
                    r = (g * pairs + i) * experts + e
                    picks[r:r + 1, :] = jnp.sum(hit.astype(F32), axis=0, keepdims=True)
                    codes[g, experts + e:experts + e + 1, i * 2 * rows:(i + 1) * 2 * rows] = jnp.sum(jnp.where(hit, gts, 0.0), axis=0, keepdims=True)
        a = lax.broadcasted_iota(jnp.int32, (2 * rows, 2 * rows), 0)
        b = lax.broadcasted_iota(jnp.int32, (2 * rows, 2 * rows), 1)
        before = ((a < b) & ((a >= rows) == (b >= rows))).astype(F32).astype(BF16)
        rank = jnp.dot(picks[...].astype(BF16), before, preferred_element_type=F32)
        for g in range(2):
            for i in range(pairs):
                start = (2 * i * cap + jnp.where(lane >= rows, cap, 0)).astype(F32)
                for e in range(experts):
                    r = (g * pairs + i) * experts + e
                    code = jnp.where(picks[r:r + 1, :] > 0.5, rank[r:r + 1, :] + start, ABSENT)
                    codes[g, e:e + 1, i * 2 * rows:(i + 1) * 2 * rows] = code
        slot = lax.broadcasted_iota(jnp.int32, (slots, group_rows), 0).astype(F32)
        col = lax.broadcasted_iota(jnp.int32, (2 * rows, experts * slots), 1).astype(F32)
        for g in range(2):
            for e in range(experts):
                pick_mat[g, e * slots:(e + 1) * slots, :] = jnp.where(slot == codes[g, e:e + 1, :], 1.0, 0.0).astype(BF16)
            for i in range(pairs):
                ct = jnp.transpose(codes[g, :, i * 2 * rows:(i + 1) * 2 * rows])
                acc = jnp.zeros((2 * rows, experts * slots), F32)
                for e in range(experts):
                    acc = jnp.where(col == ct[:, e:e + 1] + float(e * slots), ct[:, experts + e:experts + e + 1], acc)
                gate_mat[g, i * 2 * rows:(i + 1) * 2 * rows, :] = acc.astype(BF16)

    def gather(w, g, part):
        cc = c if g == 0 else 1 - c
        xs = x_all[w, pl.ds(pl.multiple_of(cc * group_rows, group_rows), group_rows), :]
        got = jnp.dot(pick_mat[g], xs, preferred_element_type=F32).astype(BF16)
        for e in range(experts):
            xg[e, g * slots:(g + 1) * slots, part * COLS:(part + 1) * COLS] = got[e * slots:(e + 1) * slots, :]

    ag_span = (hops - 1) * AG_LAG

    def in_step(j, carry):
        for k in range(hops - 1, 0, -1):
            w = j - (k - 1) * AG_LAG

            @pl.when((w >= 0) & (w < nc))
            def _():
                for up in (True, False):
                    ag_arrival(w, k, up).wait_recv()
                    ag_copy(w, k + 1, up).start()
                ag_push(w, chip(-k)).start()
                ag_push(w, chip(k)).start()

                @pl.when(w == 0)
                def _():
                    for up in (True, False):
                        tab_copy(k, up, True).wait_recv()
                        tab_copy(k + 1, up, False).start()
                    tab_push(chip(-k)).start()
                    tab_push(chip(k)).start()

        w = j + LEAD

        @pl.when(w < nc)
        def _():
            ag_copy(w, 1, True).start()
            ag_copy(w, 1, False).start()
            ag_push(w, z).start()

        for q in range(2):
            v = 2 * j + q

            @pl.when(v < nc)
            def _():
                si_copy(v).wait()
                mine = x_all[v, pl.ds(pl.multiple_of((c * chips + z) * rows, rows), rows), :]
                part = jnp.dot(mine, si_buf[v % 2], preferred_element_type=F32)

                @pl.when(v == 0)
                def _():
                    sacc[...] = part

                @pl.when(v > 0)
                def _():
                    sacc[...] += part

                @pl.when(v + 2 < nc)
                def _():
                    si_copy(v + 2).start()

        w = j - ag_span

        @pl.when((w >= 0) & (w < nc))
        def _():
            for up in (True, False):
                ag_arrival(w, hops, up).wait_recv()
            ag_push(w, chip(hops)).start()

            @pl.when(w == 0)
            def _():
                for up in (True, False):
                    tab_copy(hops, up, True).wait_recv()
                tab_push(chip(hops)).start()
                theirs = tabs.at[pl.ds((1 - c) * chips, chips)]
                pltpu.make_async_copy(theirs, theirs, tab_part).wait()
                build_tables()

        @pl.when((w >= 0) & (w < nc) & (w % PAIR == PAIR - 1))
        def _():
            m = w // PAIR
            for part in range(PAIR):
                gather(m * PAIR + part, 0, part)
            for part in range(PAIR):
                v = m * PAIR + part
                theirs = x_all.at[v, pl.ds(pl.multiple_of((1 - c) * group_rows, group_rows), group_rows)]
                pltpu.make_async_copy(theirs, theirs, ag_part.at[v]).wait()
                gather(v, 1, part)
            wi_copy(m).wait()

            @pl.when(w < nc - 1)
            def _():
                for e in range(experts):
                    hacc[e] += jnp.dot(xg[e], wi_buf[m % 2, e], preferred_element_type=F32)

            @pl.when(w == nc - 1)
            def _():
                for e in range(experts):
                    h[e] = gelu(hacc[e] + jnp.dot(xg[e], wi_buf[m % 2, e], preferred_element_type=F32)).astype(BF16)

            @pl.when(m + 2 < nc // PAIR)
            def _():
                wi_copy(m + 2).start()

        return carry

    lax.fori_loop(0, nc + ag_span, in_step, 0)

    s_act[...] = gelu(sacc[...]).astype(BF16)

    def prow(w, s, lo=0, count=None):
        return pbuf.at[w, pl.ds(pl.multiple_of(s * rows + lo, half), rows if count is None else count)]

    def rs_copy(w, k, up):
        off = hops - k + 1
        s = chip(off) if up else chip(-off)
        lo, cnt = (0, rows) if k > 1 else ((0, half) if up else (half, half))
        d = 0 if up else 1
        return remote(prow(w, s, lo, cnt), rbuf.at[d, w, k - 1, pl.ds(lo, cnt)], rs_send.at[w], rs_recv.at[d, w, k - 1], nxt if up else prv)

    def push_copy(w):
        return remote(ppush.at[w % 2], prec.at[w % 2], pp_send.at[w % 2], pp_recv.at[w % 2], partner)

    def out_step(i, carry):
        @pl.when(i < nc)
        def _():
            wo_copy(i).wait()
            for e in range(experts):
                o = jnp.dot(h[e], wo_buf[i % 2, e], preferred_element_type=F32).astype(BF16)
                outs[0, e * slots:(e + 1) * slots, :] = o[:slots]
                outs[1, e * slots:(e + 1) * slots, :] = o[slots:]

            @pl.when(i >= 2)
            def _():
                push_copy(i).wait_send()

            ppush[i % 2] = jnp.dot(gate_mat[1], outs[1], preferred_element_type=F32)
            push_copy(i).start()
            pbuf[i] = jnp.dot(gate_mat[0], outs[0], preferred_element_type=F32)
            so_copy(i).wait()
            u_all[i] = jnp.dot(s_act[...], so_buf[i % 2], preferred_element_type=F32)

            @pl.when(i + 2 < nc)
            def _():
                wo_copy(i + 2).start()
                so_copy(i + 2).start()

        for k in range(hops - 1, 0, -1):
            w = i - k * RS_LAG

            @pl.when((w >= 0) & (w < nc))
            def _():
                for up in (True, False):
                    rs_copy(w, k, up).wait_recv()
                    d = 0 if up else 1
                    s = chip(hops - k) if up else chip(-(hops - k))
                    lo, cnt = (0, rows) if k > 1 else ((0, half) if up else (half, half))
                    dst = prow(w, s, lo, cnt)
                    dst[...] += rbuf[d, w, k - 1, lo:lo + cnt, :]
                    rs_copy(w, k + 1, up).start()

        @pl.when(i < nc)
        def _():
            push_copy(i).wait_recv()
            pbuf[i] += prec[i % 2]
            rs_copy(i, 1, True).start()
            rs_copy(i, 1, False).start()

        w = i - hops * RS_LAG

        @pl.when(w >= 0)
        def _():
            rs_copy(w, hops, True).wait_recv()
            rs_copy(w, hops, False).wait_recv()
            total = prow(w, z)[...] + (rbuf[0, w, hops - 1] + rbuf[1, w, hops - 1]) + u_all[w]
            y_ref[:, pl.ds(pl.multiple_of(w * COLS, COLS), COLS)] = total.astype(BF16)

        return carry

    lax.fori_loop(0, nc + hops * RS_LAG, out_step, 0)

    def drain(w, carry):
        sent = x_all.at[w, pl.ds(0, (2 * chips - 1) * rows)]
        pltpu.make_async_copy(sent, sent, ag_send.at[w]).wait()
        sums = pbuf.at[w, pl.ds(0, (chips - 1) * rows)]
        pltpu.make_async_copy(sums, sums, rs_send.at[w]).wait()
        return carry

    lax.fori_loop(0, nc, drain, 0)
    sent = tabs.at[pl.ds(0, 2 * chips - 1)]
    pltpu.make_async_copy(sent, sent, tab_send).wait()
    for w in range(min(2, nc)):
        push_copy(w).wait_send()


def solution(mesh):
    group_size = mesh.shape['ep']
    chips = group_size // CORES
    hops = chips // 2

    def local_layer(x_loc, idx_loc, gate_loc, w_in, w_out, shared_in, shared_out):
        rows, top_k = idx_loc.shape
        d_model = x_loc.shape[1]
        experts, _, ff = w_in.shape
        fs = shared_in.shape[1]
        num_experts = experts * group_size
        cap = min(rows, LOAD_MULT * rows * top_k // num_experts)
        slots = chips * cap
        nc = d_model // COLS
        any_spec = pl.BlockSpec(memory_space=pl.ANY)
        dma = pltpu.SemaphoreType.DMA
        flops = 2 * group_size * cap * experts * d_model * ff * 2
        return pl.pallas_call(
            functools.partial(moe_kernel, chips, cap, top_k),
            out_shape=jax.ShapeDtypeStruct((rows, d_model), BF16),
            in_specs=[any_spec] * 7,
            out_specs=pl.BlockSpec(memory_space=pltpu.VMEM),
            scratch_shapes=[
                pltpu.VMEM((nc, group_size * rows, COLS), BF16),
                pltpu.VMEM((top_k, rows), jnp.int32),
                pltpu.VMEM((top_k, rows), F32),
                pltpu.VMEM((group_size, 16, 2 * rows), F32),
                pltpu.VMEM((chips * experts, 2 * rows), F32),
                pltpu.VMEM((2, 2 * experts, chips * rows), F32),
                pltpu.VMEM((2, experts * slots, chips * rows), BF16),
                pltpu.VMEM((2, chips * rows, experts * slots), BF16),
                pltpu.VMEM((experts, 2 * slots, PAIR * COLS), BF16),
                pltpu.VMEM((experts, 2 * slots, ff), F32),
                pltpu.VMEM((experts, 2 * slots, ff), BF16),
                pltpu.VMEM((2, experts * slots, COLS), BF16),
                pltpu.VMEM((nc, chips * rows, COLS), F32),
                pltpu.VMEM((2, chips * rows, COLS), F32),
                pltpu.VMEM((2, chips * rows, COLS), F32),
                pltpu.VMEM((2, nc, hops, rows, COLS), F32),
                pltpu.VMEM((rows, fs), F32),
                pltpu.VMEM((rows, fs), BF16),
                pltpu.VMEM((nc, rows, COLS), F32),
                pltpu.VMEM((2, experts, PAIR * COLS, ff), BF16),
                pltpu.VMEM((2, experts, ff, COLS), BF16),
                pltpu.VMEM((2, COLS, fs), BF16),
                pltpu.VMEM((2, fs, COLS), BF16),
                dma((2, nc, hops)), dma((2, hops)), dma((nc,)), dma(()), dma((nc,)), dma(()), dma((3,)),
                dma((2, nc, hops)), dma((nc,)), dma((2,)), dma((2,)),
                dma((2,)), dma((2,)), dma((2,)), dma((2,)),
            ],
            compiler_params=pltpu.CompilerParams(collective_id=0, has_side_effects=True, vmem_limit_bytes=VMEM_BYTES),
            cost_estimate=pl.CostEstimate(flops=flops, bytes_accessed=2 * (w_in.size + w_out.size + shared_in.size + shared_out.size), transcendentals=0),
        )(x_loc, idx_loc.T, gate_loc.T, w_in, w_out, shared_in, shared_out)

    tok_spec = P(('dp', 'ep'), None)
    expert_spec = P('ep', None, None)
    whole_spec = P(None, None)
    return jax.shard_map(local_layer, mesh=mesh, in_specs=(tok_spec, tok_spec, tok_spec, expert_spec, expert_spec, whole_spec, whole_spec), out_specs=tok_spec, check_vma=False)
```

```python
import functools

import jax
import jax.numpy as jnp
from jax import lax
from jax.experimental import pallas as pl
from jax.experimental.pallas import tpu as pltpu
from jax.sharding import PartitionSpec as P

LOAD_MULT = 3
COLS = 256
LEAD = 4
AG_LAG = 2
RS_LAGS = (1, 3, 5, 9, 11)
PAIR = 2
SI_SLOTS = 4
SI_EARLY = 4
CORES = 2
ABSENT = -4096.0
VMEM_BYTES = 67_000_000
F32 = jnp.float32
BF16 = jnp.bfloat16


def gelu(z):
    return 0.5 * z * (1.0 + jnp.tanh(0.7978845608028654 * (z + 0.044715 * (z * z * z))))


def moe_kernel(chips, cap, top_k,
               x_hbm, idx_hbm, top_hbm, wi_hbm, wo_hbm, si_hbm, so_hbm, y_ref,
               x_all, idx_v, top_v, tabs, picks, codes, pick_mat, gate_mat, xg, hacc, h, outs, pbuf, part, ppush, rbuf,
               sacc, s_act, u_all, wi_buf, wo_buf, si_buf, so_buf,
               ag_recv, tab_recv, ag_part, tab_part, ag_send, tab_send, own_sem,
               rs_recv, rs_send, pp_send, pp_recv, wi_sem, wo_sem, si_sem, so_sem):
    rows, d_model = x_hbm.shape
    experts = wi_hbm.shape[0]
    nc = d_model // COLS
    hops = chips // 2
    half = rows // 2
    group_rows = chips * rows
    slots = chips * cap

    ep = lax.axis_index('ep')
    z, c = ep // CORES, ep % CORES
    first = lax.axis_index('dp') * (chips * CORES)
    partner = first + z * CORES + (1 - c)
    nxt = first + ((z + 1) % chips) * CORES + c
    prv = first + ((z + chips - 1) % chips) * CORES + c
    near = [(z + off) % chips for off in range(chips)]

    def chip(off):
        return near[off % chips]

    def xrows(w, s, lo=0, count=None):
        base = (c * chips + s) * rows + lo
        return x_all.at[w, pl.ds(pl.multiple_of(base, half), rows if count is None else count)]

    def tblk(s, lo=0, count=None):
        t = tabs.at[c * chips + s]
        return t if count is None else t.at[pl.ds(lo, count)]

    def remote(src, dst, ssem, rsem, dev):
        return pltpu.make_async_remote_copy(src_ref=src, dst_ref=dst, send_sem=ssem, recv_sem=rsem, device_id=dev, device_id_type=pl.DeviceIdType.LOGICAL)

    def ag_copy(w, k, up):
        s = chip(-(k - 1)) if up else chip(k - 1)
        lo, cnt = (0, None) if k < hops else ((0, half) if up else (half, half))
        ref = xrows(w, s, lo, cnt)
        return remote(ref, ref, ag_send.at[w], ag_recv.at[0 if up else 1, w, k - 1], nxt if up else prv)

    def ag_arrival(w, k, up):
        s = chip(-k) if up else chip(k)
        lo, cnt = (0, None) if k < hops else ((0, half) if up else (half, half))
        ref = xrows(w, s, lo, cnt)
        return remote(ref, ref, ag_send.at[w], ag_recv.at[0 if up else 1, w, k - 1], nxt if up else prv)

    def tab_copy(k, up, arrival):
        off = k if arrival else k - 1
        s = chip(-off) if up else chip(off)
        lo, cnt = (0, None) if k < hops else ((0, 8) if up else (8, 8))
        ref = tblk(s, lo, cnt)
        return remote(ref, ref, tab_send, tab_recv.at[0 if up else 1, k - 1], nxt if up else prv)

    def ag_push(w, s):
        ref = xrows(w, s)
        return remote(ref, ref, ag_send.at[w], ag_part.at[w], partner)

    def tab_push(s):
        ref = tblk(s)
        return remote(ref, ref, tab_send, tab_part, partner)

    def wi_copy(w):
        return pltpu.make_async_copy(wi_hbm.at[:, pl.ds(pl.multiple_of(w * PAIR * COLS, COLS), PAIR * COLS), :], wi_buf.at[w % 2], wi_sem.at[w % 2])

    def wo_copy(w):
        return pltpu.make_async_copy(wo_hbm.at[:, :, pl.ds(pl.multiple_of(w * COLS, COLS), COLS)], wo_buf.at[w % 2], wo_sem.at[w % 2])

    def si_copy(w):
        return pltpu.make_async_copy(si_hbm.at[pl.ds(pl.multiple_of(w * COLS, COLS), COLS), :], si_buf.at[w % SI_SLOTS], si_sem.at[w % SI_SLOTS])

    def so_copy(w):
        return pltpu.make_async_copy(so_hbm.at[:, pl.ds(pl.multiple_of(w * COLS, COLS), COLS)], so_buf.at[w % 2], so_sem.at[w % 2])

    for w in range(nc):
        pltpu.make_async_copy(x_hbm.at[:, pl.ds(w * COLS, COLS)], xrows(w, z), own_sem.at[0]).start()
    pltpu.make_async_copy(idx_hbm, idx_v, own_sem.at[1]).start()
    pltpu.make_async_copy(top_hbm, top_v, own_sem.at[2]).start()
    for w in range(min(SI_SLOTS, nc)):
        si_copy(w).start()

    barrier = pltpu.get_barrier_semaphore()
    for dev in (nxt, prv, partner):
        pl.semaphore_signal(barrier, inc=1, device_id=dev, device_id_type=pl.DeviceIdType.LOGICAL)
    pl.semaphore_wait(barrier, 3)

    pltpu.make_async_copy(idx_hbm, idx_v, own_sem.at[1]).wait()
    pltpu.make_async_copy(top_hbm, top_v, own_sem.at[2]).wait()
    right = lax.broadcasted_iota(jnp.int32, (top_k, 2 * rows), 1) >= rows
    side = right == (z % 2 == 1)
    ids, gts = idx_v[...].astype(F32), top_v[...]
    mine = tabs.at[c * chips + z]
    mine[...] = jnp.zeros_like(mine)
    mine[0:top_k, :] = jnp.where(side, jnp.concatenate([ids, ids], axis=1), 0.0)
    mine[8:8 + top_k, :] = jnp.where(side, jnp.concatenate([gts, gts], axis=1), 0.0)
    own_all = x_all.at[0, pl.ds(0, nc * rows)]
    pltpu.make_async_copy(own_all, own_all, own_sem.at[0]).wait()
    for w in range(min(LEAD, nc)):
        ag_copy(w, 1, True).start()
        ag_copy(w, 1, False).start()
        if w == 0:
            tab_copy(1, True, False).start()
            tab_copy(1, False, False).start()
            tab_push(z).start()
        ag_push(w, z).start()

    def shared_in(v):
        si_copy(v).wait()
        own = x_all[v, pl.ds(pl.multiple_of((c * chips + z) * rows, rows), rows), :]
        sacc[...] += jnp.dot(own, si_buf[v % SI_SLOTS], preferred_element_type=F32)

        @pl.when(v + SI_SLOTS < nc)
        def _():
            si_copy(v + SI_SLOTS).start()

    sacc[...] = jnp.zeros_like(sacc)

    def early_step(v, carry):
        shared_in(v)
        return carry

    lax.fori_loop(0, SI_EARLY, early_step, 0)
    wi_copy(0).start()
    hacc[...] = jnp.zeros_like(hacc)

    def build_tables():
        base = (ep * experts).astype(F32)
        lane = lax.broadcasted_iota(jnp.int32, (1, 2 * rows), 1)
        pairs = chips // 2
        for g in range(2):
            cc = c if g == 0 else 1 - c
            for i in range(pairs):
                t = tabs[cc * chips + 2 * i] + tabs[cc * chips + 2 * i + 1]
                ids, gts = t[0:top_k], t[8:8 + top_k]
                for e in range(experts):
                    hit = ids == (base + float(e))
                    r = (g * pairs + i) * experts + e
                    picks[r:r + 1, :] = jnp.sum(hit.astype(F32), axis=0, keepdims=True)
                    codes[g, experts + e:experts + e + 1, i * 2 * rows:(i + 1) * 2 * rows] = jnp.sum(jnp.where(hit, gts, 0.0), axis=0, keepdims=True)
        a = lax.broadcasted_iota(jnp.int32, (2 * rows, 2 * rows), 0)
        b = lax.broadcasted_iota(jnp.int32, (2 * rows, 2 * rows), 1)
        before = ((a < b) & ((a >= rows) == (b >= rows))).astype(F32).astype(BF16)
        rank = jnp.dot(picks[...].astype(BF16), before, preferred_element_type=F32)
        for g in range(2):
            for i in range(pairs):
                start = (2 * i * cap + jnp.where(lane >= rows, cap, 0)).astype(F32)
                for e in range(experts):
                    r = (g * pairs + i) * experts + e
                    code = jnp.where(picks[r:r + 1, :] > 0.5, rank[r:r + 1, :] + start, ABSENT)
                    codes[g, e:e + 1, i * 2 * rows:(i + 1) * 2 * rows] = code
        slot = lax.broadcasted_iota(jnp.int32, (slots, group_rows), 0).astype(F32)
        col = lax.broadcasted_iota(jnp.int32, (2 * rows, experts * slots), 1).astype(F32)
        for g in range(2):
            for e in range(experts):
                pick_mat[g, e * slots:(e + 1) * slots, :] = jnp.where(slot == codes[g, e:e + 1, :], 1.0, 0.0).astype(BF16)
            for i in range(pairs):
                ct = jnp.transpose(codes[g, :, i * 2 * rows:(i + 1) * 2 * rows])
                acc = jnp.zeros((2 * rows, experts * slots), F32)
                for e in range(experts):
                    acc = jnp.where(col == ct[:, e:e + 1] + float(e * slots), ct[:, experts + e:experts + e + 1], acc)
                gate_mat[g, i * 2 * rows:(i + 1) * 2 * rows, :] = acc.astype(BF16)

    def gather(w, g, part):
        cc = c if g == 0 else 1 - c
        xs = x_all[w, pl.ds(pl.multiple_of(cc * group_rows, group_rows), group_rows), :]
        got = jnp.dot(pick_mat[g], xs, preferred_element_type=F32).astype(BF16)
        for e in range(experts):
            xg[e, g * slots:(g + 1) * slots, part * COLS:(part + 1) * COLS] = got[e * slots:(e + 1) * slots, :]

    ag_span = (hops - 1) * AG_LAG

    def expert_in(m, lo):
        @pl.when(m < nc // PAIR - 1)
        def _():
            for e in range(lo, lo + experts // 2):
                hacc[e] += jnp.dot(xg[e], wi_buf[m % 2, e], preferred_element_type=F32)

        @pl.when(m == nc // PAIR - 1)
        def _():
            for e in range(lo, lo + experts // 2):
                h[e] = gelu(hacc[e] + jnp.dot(xg[e], wi_buf[m % 2, e], preferred_element_type=F32)).astype(BF16)

    def in_step(j, carry):
        for k in range(1, hops):
            w = j - (k - 1) * AG_LAG

            @pl.when((w >= 0) & (w < nc))
            def _():
                for up in (True, False):
                    ag_arrival(w, k, up).wait_recv()
                    ag_copy(w, k + 1, up).start()
                ag_push(w, chip(-k)).start()
                ag_push(w, chip(k)).start()

                @pl.when(w == 0)
                def _():
                    for up in (True, False):
                        tab_copy(k, up, True).wait_recv()
                        tab_copy(k + 1, up, False).start()
                    tab_push(chip(-k)).start()
                    tab_push(chip(k)).start()

        w = j + LEAD

        @pl.when(w < nc)
        def _():
            ag_copy(w, 1, True).start()
            ag_copy(w, 1, False).start()
            ag_push(w, z).start()

        @pl.when(j == 3)
        def _():
            wi_copy(1).start()

        @pl.when(j == 7)
        def _():
            for v in range(2):
                wo_copy(v).start()
                so_copy(v).start()

        @pl.when(j + SI_EARLY < nc)
        def _():
            shared_in(j + SI_EARLY)

        w = j - ag_span

        @pl.when((w >= 0) & (w < nc))
        def _():
            for up in (True, False):
                ag_arrival(w, hops, up).wait_recv()
            ag_push(w, chip(hops)).start()

            @pl.when(w == 0)
            def _():
                for up in (True, False):
                    tab_copy(hops, up, True).wait_recv()
                tab_push(chip(hops)).start()
                theirs = tabs.at[pl.ds((1 - c) * chips, chips)]
                pltpu.make_async_copy(theirs, theirs, tab_part).wait()
                build_tables()

        @pl.when((w >= 0) & (w < nc) & (w % PAIR == PAIR - 1))
        def _():
            m = w // PAIR
            for part in range(PAIR):
                gather(m * PAIR + part, 0, part)
            for part in range(PAIR):
                v = m * PAIR + part
                theirs = x_all.at[v, pl.ds(pl.multiple_of((1 - c) * group_rows, group_rows), group_rows)]
                pltpu.make_async_copy(theirs, theirs, ag_part.at[v]).wait()
                gather(v, 1, part)
            wi_copy(m).wait()
            expert_in(m, 0)

        v = w - 1

        @pl.when((v >= 0) & (v < nc) & (v % PAIR == PAIR - 1))
        def _():
            m = v // PAIR
            expert_in(m, experts // 2)

            @pl.when(m + 2 < nc // PAIR)
            def _():
                wi_copy(m + 2).start()

        return carry

    lax.fori_loop(0, nc + ag_span + 1, in_step, 0)

    s_act[...] = gelu(sacc[...]).astype(BF16)

    def prow(w, s, lo=0, count=None):
        return pbuf.at[w, pl.ds(pl.multiple_of(s * rows + lo, half), rows if count is None else count)]

    def rs_copy(w, k, up):
        off = hops - k + 1
        s = chip(off) if up else chip(-off)
        lo, cnt = (0, rows) if k > 1 else ((0, half) if up else (half, half))
        d = 0 if up else 1
        return remote(prow(w, s, lo, cnt), rbuf.at[d, w, k - 1, pl.ds(lo, cnt)], rs_send.at[w], rs_recv.at[d, w, k - 1], nxt if up else prv)

    def push_copy(w):
        return remote(ppush.at[w % 2], pbuf.at[w], pp_send.at[w % 2], pp_recv.at[w], partner)

    def out_step(i, carry):
        for k in range(hops - 1, 0, -1):
            w = i - RS_LAGS[k]

            @pl.when((w >= 0) & (w < nc))
            def _():
                for up in (True, False):
                    rs_copy(w, k, up).wait_recv()
                    d = 0 if up else 1
                    s = chip(hops - k) if up else chip(-(hops - k))
                    lo, cnt = (0, rows) if k > 1 else ((0, half) if up else (half, half))
                    dst = prow(w, s, lo, cnt)
                    dst[...] += rbuf[d, w, k - 1, lo:lo + cnt, :]
                    rs_copy(w, k + 1, up).start()

        @pl.when(i < nc)
        def _():
            wo_copy(i).wait()
            for e in range(experts):
                o = jnp.dot(h[e], wo_buf[i % 2, e], preferred_element_type=F32).astype(BF16)
                outs[0, e * slots:(e + 1) * slots, :] = o[:slots]
                outs[1, e * slots:(e + 1) * slots, :] = o[slots:]

            @pl.when(i >= 2)
            def _():
                push_copy(i).wait_send()

            ppush[i % 2] = jnp.dot(gate_mat[1], outs[1], preferred_element_type=F32)
            push_copy(i).start()
            part[i % 2] = jnp.dot(gate_mat[0], outs[0], preferred_element_type=F32)
            so_copy(i).wait()
            u_all[i] = jnp.dot(s_act[...], so_buf[i % 2], preferred_element_type=F32)

            @pl.when(i + 2 < nc)
            def _():
                wo_copy(i + 2).start()
                so_copy(i + 2).start()

        w = i - RS_LAGS[0]

        @pl.when((w >= 0) & (w < nc))
        def _():
            push_copy(w).wait_recv()
            pbuf[w] += part[w % 2]
            rs_copy(w, 1, True).start()
            rs_copy(w, 1, False).start()

        w = i - RS_LAGS[hops]

        @pl.when(w >= 0)
        def _():
            rs_copy(w, hops, True).wait_recv()
            rs_copy(w, hops, False).wait_recv()
            total = prow(w, z)[...] + (rbuf[0, w, hops - 1] + rbuf[1, w, hops - 1]) + u_all[w]
            y_ref[:, pl.ds(pl.multiple_of(w * COLS, COLS), COLS)] = total.astype(BF16)

        return carry

    lax.fori_loop(0, nc + RS_LAGS[hops], out_step, 0)

    def drain(w, carry):
        sent = x_all.at[w, pl.ds(0, (2 * chips - 1) * rows)]
        pltpu.make_async_copy(sent, sent, ag_send.at[w]).wait()
        sums = pbuf.at[w, pl.ds(0, (chips - 1) * rows)]
        pltpu.make_async_copy(sums, sums, rs_send.at[w]).wait()
        return carry

    lax.fori_loop(0, nc, drain, 0)
    sent = tabs.at[pl.ds(0, 2 * chips - 1)]
    pltpu.make_async_copy(sent, sent, tab_send).wait()
    for w in range(min(2, nc)):
        push_copy(w).wait_send()


def solution(mesh):
    group_size = mesh.shape['ep']
    chips = group_size // CORES
    hops = chips // 2

    def local_layer(x_loc, idx_loc, gate_loc, w_in, w_out, shared_in, shared_out):
        rows, top_k = idx_loc.shape
        d_model = x_loc.shape[1]
        experts, _, ff = w_in.shape
        fs = shared_in.shape[1]
        num_experts = experts * group_size
        cap = min(rows, LOAD_MULT * rows * top_k // num_experts)
        slots = chips * cap
        nc = d_model // COLS
        any_spec = pl.BlockSpec(memory_space=pl.ANY)
        dma = pltpu.SemaphoreType.DMA
        flops = 2 * group_size * cap * experts * d_model * ff * 2
        return pl.pallas_call(
            functools.partial(moe_kernel, chips, cap, top_k),
            out_shape=jax.ShapeDtypeStruct((rows, d_model), BF16),
            in_specs=[any_spec] * 7,
            out_specs=pl.BlockSpec(memory_space=pltpu.VMEM),
            scratch_shapes=[
                pltpu.VMEM((nc, group_size * rows, COLS), BF16),
                pltpu.VMEM((top_k, rows), jnp.int32),
                pltpu.VMEM((top_k, rows), F32),
                pltpu.VMEM((group_size, 16, 2 * rows), F32),
                pltpu.VMEM((chips * experts, 2 * rows), F32),
                pltpu.VMEM((2, 2 * experts, chips * rows), F32),
                pltpu.VMEM((2, experts * slots, chips * rows), BF16),
                pltpu.VMEM((2, chips * rows, experts * slots), BF16),
                pltpu.VMEM((experts, 2 * slots, PAIR * COLS), BF16),
                pltpu.VMEM((experts, 2 * slots, ff), F32),
                pltpu.VMEM((experts, 2 * slots, ff), BF16),
                pltpu.VMEM((2, experts * slots, COLS), BF16),
                pltpu.VMEM((nc, chips * rows, COLS), F32),
                pltpu.VMEM((2, chips * rows, COLS), F32),
                pltpu.VMEM((2, chips * rows, COLS), F32),
                pltpu.VMEM((2, nc, hops, rows, COLS), F32),
                pltpu.VMEM((rows, fs), F32),
                pltpu.VMEM((rows, fs), BF16),
                pltpu.VMEM((nc, rows, COLS), F32),
                pltpu.VMEM((2, experts, PAIR * COLS, ff), BF16),
                pltpu.VMEM((2, experts, ff, COLS), BF16),
                pltpu.VMEM((SI_SLOTS, COLS, fs), BF16),
                pltpu.VMEM((2, fs, COLS), BF16),
                dma((2, nc, hops)), dma((2, hops)), dma((nc,)), dma(()), dma((nc,)), dma(()), dma((3,)),
                dma((2, nc, hops)), dma((nc,)), dma((2,)), dma((nc,)),
                dma((2,)), dma((2,)), dma((SI_SLOTS,)), dma((2,)),
            ],
            compiler_params=pltpu.CompilerParams(collective_id=0, has_side_effects=True, vmem_limit_bytes=VMEM_BYTES),
            cost_estimate=pl.CostEstimate(flops=flops, bytes_accessed=2 * (w_in.size + w_out.size + shared_in.size + shared_out.size), transcendentals=0),
        )(x_loc, idx_loc.T, gate_loc.T, w_in, w_out, shared_in, shared_out)

    tok_spec = P(('dp', 'ep'), None)
    expert_spec = P('ep', None, None)
    whole_spec = P(None, None)
    return jax.shard_map(local_layer, mesh=mesh, in_specs=(tok_spec, tok_spec, tok_spec, expert_spec, expert_spec, whole_spec, whole_spec), out_specs=tok_spec, check_vma=False)
```

```python
import functools

import jax
import jax.numpy as jnp
from jax import lax
from jax.experimental import pallas as pl
from jax.experimental.pallas import tpu as pltpu
from jax.sharding import PartitionSpec as P

LOAD_MULT = 3
COLS = 256
LEAD = 5
AG_LAGS = (0, 4, 8, 12)
AG_SHIFT = 12
RS_LAGS = (0, 2, 4, 9, 17)
PAIR = 2
IN_FIRST = 15
OUT_OFF = 0
SI_SLOTS = 4
SI_EARLY = 2
WI_AT, SO_AT, WO_AT = 3, 8, 14
CORES = 2
ABSENT = -4096.0
VMEM_BYTES = 67_000_000
F32 = jnp.float32
BF16 = jnp.bfloat16


def gelu(z):
    return 0.5 * z * (1.0 + jnp.tanh(0.7978845608028654 * (z + 0.044715 * (z * z * z))))


def moe_kernel(chips, cap, top_k,
               x_hbm, idx_hbm, top_hbm, wi_hbm, wo_hbm, si_hbm, so_hbm, y_ref,
               x_all, idx_v, top_v, tabs, picks, codes, pick_mat, gate_mat, xg, hacc, h, outs, pbuf, part, rbuf,
               sacc, s_act, u_all, wi_buf, wo_buf, si_buf, so_buf,
               ag_recv, tab_recv, ag_part, tab_part, ag_send, tab_send, own_sem,
               rs_recv, rs_send, pp_send, pp_recv, wi_sem, wo_sem, si_sem, so_sem):
    rows, d_model = x_hbm.shape
    experts = wi_hbm.shape[0]
    nc = d_model // COLS
    hops = chips // 2
    pairs_in = nc // PAIR
    half = rows // 2
    group_rows = chips * rows
    slots = chips * cap

    ep = lax.axis_index('ep')
    z, c = ep // CORES, ep % CORES
    first = lax.axis_index('dp') * (chips * CORES)
    partner = first + z * CORES + (1 - c)
    nxt = first + ((z + 1) % chips) * CORES + c
    prv = first + ((z + chips - 1) % chips) * CORES + c
    near = [(z + off) % chips for off in range(chips)]

    def chip(off):
        return near[off % chips]

    def xrows(w, s, lo=0, count=None):
        base = (c * chips + s) * rows + lo
        return x_all.at[w, pl.ds(pl.multiple_of(base, half), rows if count is None else count)]

    def tblk(s, lo=0, count=None):
        t = tabs.at[c * chips + s]
        return t if count is None else t.at[pl.ds(lo, count)]

    def remote(src, dst, ssem, rsem, dev):
        return pltpu.make_async_remote_copy(src_ref=src, dst_ref=dst, send_sem=ssem, recv_sem=rsem, device_id=dev, device_id_type=pl.DeviceIdType.LOGICAL)

    def ag_copy(w, k, up):
        s = chip(-(k - 1)) if up else chip(k - 1)
        lo, cnt = (0, None) if k < hops else ((0, half) if up else (half, half))
        ref = xrows(w, s, lo, cnt)
        return remote(ref, ref, ag_send.at[w], ag_recv.at[0 if up else 1, w, k - 1], nxt if up else prv)

    def ag_arrival(w, k, up):
        s = chip(-k) if up else chip(k)
        lo, cnt = (0, None) if k < hops else ((0, half) if up else (half, half))
        ref = xrows(w, s, lo, cnt)
        return remote(ref, ref, ag_send.at[w], ag_recv.at[0 if up else 1, w, k - 1], nxt if up else prv)

    def tab_copy(k, up, arrival):
        off = k if arrival else k - 1
        s = chip(-off) if up else chip(off)
        lo, cnt = (0, None) if k < hops else ((0, 8) if up else (8, 8))
        ref = tblk(s, lo, cnt)
        return remote(ref, ref, tab_send, tab_recv.at[0 if up else 1, k - 1], nxt if up else prv)

    def ag_push(w, s):
        ref = xrows(w, s)
        return remote(ref, ref, ag_send.at[w], ag_part.at[w], partner)

    def tab_push(s):
        ref = tblk(s)
        return remote(ref, ref, tab_send, tab_part, partner)

    def wi_copy(w):
        return pltpu.make_async_copy(wi_hbm.at[:, pl.ds(pl.multiple_of(w % pairs_in * (PAIR * COLS), COLS), PAIR * COLS), :], wi_buf.at[w % 2], wi_sem.at[w % 2])

    def wo_copy(w):
        return pltpu.make_async_copy(wo_hbm.at[:, :, pl.ds(pl.multiple_of(w % nc * COLS, COLS), COLS)], wo_buf.at[w % 2], wo_sem.at[w % 2])

    def si_copy(w):
        return pltpu.make_async_copy(si_hbm.at[pl.ds(pl.multiple_of(w * COLS, COLS), COLS), :], si_buf.at[w % SI_SLOTS], si_sem.at[w % SI_SLOTS])

    def so_copy(w):
        return pltpu.make_async_copy(so_hbm.at[:, pl.ds(pl.multiple_of(w * COLS, COLS), COLS)], so_buf.at[w % 2], so_sem.at[w % 2])

    for w in range(nc):
        pltpu.make_async_copy(x_hbm.at[:, pl.ds(w * COLS, COLS)], xrows(w, z), own_sem.at[0]).start()
    pltpu.make_async_copy(idx_hbm, idx_v, own_sem.at[1]).start()
    pltpu.make_async_copy(top_hbm, top_v, own_sem.at[2]).start()
    for w in range(min(SI_SLOTS, nc)):
        si_copy(w).start()

    barrier = pltpu.get_barrier_semaphore()
    for dev in (nxt, prv, partner):
        pl.semaphore_signal(barrier, inc=1, device_id=dev, device_id_type=pl.DeviceIdType.LOGICAL)
    pl.semaphore_wait(barrier, 3)

    pltpu.make_async_copy(idx_hbm, idx_v, own_sem.at[1]).wait()
    pltpu.make_async_copy(top_hbm, top_v, own_sem.at[2]).wait()
    right = lax.broadcasted_iota(jnp.int32, (top_k, 2 * rows), 1) >= rows
    side = right == (z % 2 == 1)
    ids, gts = idx_v[...].astype(F32), top_v[...]
    mine = tabs.at[c * chips + z]
    mine[...] = jnp.zeros_like(mine)
    mine[0:top_k, :] = jnp.where(side, jnp.concatenate([ids, ids], axis=1), 0.0)
    mine[8:8 + top_k, :] = jnp.where(side, jnp.concatenate([gts, gts], axis=1), 0.0)
    own_all = x_all.at[0, pl.ds(0, nc * rows)]
    pltpu.make_async_copy(own_all, own_all, own_sem.at[0]).wait()
    def ag_own(w):
        ag_copy(w, 1, True).start()
        ag_copy(w, 1, False).start()
        ag_push(w, z).start()

    @pl.when(c == 0)
    def _():
        for w in range(min(LEAD, nc)):
            ag_own(w)

    tab_copy(1, True, False).start()
    tab_copy(1, False, False).start()
    tab_push(z).start()

    def shared_in(v):
        si_copy(v).wait()
        own = x_all[v, pl.ds(pl.multiple_of((c * chips + z) * rows, rows), rows), :]
        sacc[...] += jnp.dot(own, si_buf[v % SI_SLOTS], preferred_element_type=F32)

        @pl.when(v + SI_SLOTS < nc)
        def _():
            si_copy(v + SI_SLOTS).start()

    sacc[...] = jnp.zeros_like(sacc)

    def early_step(v, carry):
        shared_in(v)
        return carry

    lax.fori_loop(0, SI_EARLY, early_step, 0)
    wi_copy(0).start()

    def build_tables(g):
        base = (ep * experts).astype(F32)
        lane = lax.broadcasted_iota(jnp.int32, (1, 2 * rows), 1)
        pairs = chips // 2
        for i in range(pairs):
            t = tabs[g * chips + 2 * i] + tabs[g * chips + 2 * i + 1]
            ids, gts = t[0:top_k], t[8:8 + top_k]
            for e in range(experts):
                hit = ids == (base + float(e))
                r = i * experts + e
                picks[r:r + 1, :] = jnp.sum(hit.astype(F32), axis=0, keepdims=True)
                codes[experts + e:experts + e + 1, i * 2 * rows:(i + 1) * 2 * rows] = jnp.sum(jnp.where(hit, gts, 0.0), axis=0, keepdims=True)
        a = lax.broadcasted_iota(jnp.int32, (2 * rows, 2 * rows), 0)
        b = lax.broadcasted_iota(jnp.int32, (2 * rows, 2 * rows), 1)
        before = ((a < b) & ((a >= rows) == (b >= rows))).astype(F32).astype(BF16)
        rank = jnp.dot(picks[...].astype(BF16), before, preferred_element_type=F32)
        for i in range(pairs):
            start = (2 * i * cap + jnp.where(lane >= rows, cap, 0)).astype(F32)
            for e in range(experts):
                r = i * experts + e
                code = jnp.where(picks[r:r + 1, :] > 0.5, rank[r:r + 1, :] + start, ABSENT)
                codes[e:e + 1, i * 2 * rows:(i + 1) * 2 * rows] = code
        slot = lax.broadcasted_iota(jnp.int32, (slots, group_rows), 0).astype(F32)
        col = lax.broadcasted_iota(jnp.int32, (2 * rows, experts * slots), 1).astype(F32)
        for e in range(experts):
            pick_mat[g, e * slots:(e + 1) * slots, :] = jnp.where(slot == codes[e:e + 1, :], 1.0, 0.0).astype(BF16)
        for i in range(pairs):
            ct = jnp.transpose(codes[:, i * 2 * rows:(i + 1) * 2 * rows])
            acc = jnp.zeros((2 * rows, experts * slots), F32)
            for e in range(experts):
                acc = jnp.where(col == ct[:, e:e + 1] + float(e * slots), ct[:, experts + e:experts + e + 1], acc)
            gate_mat[g, i * 2 * rows:(i + 1) * 2 * rows, :] = acc.astype(BF16)

    def gather(w, g, q):
        xs = x_all[w, pl.ds(pl.multiple_of(g * group_rows, group_rows), group_rows), :]
        got = jnp.dot(pick_mat[g], xs, preferred_element_type=F32).astype(BF16)
        for e in range(experts):
            xg[e, :, q * COLS:(q + 1) * COLS] = got[e * slots:(e + 1) * slots, :]

    ag_span = AG_LAGS[hops - 1]
    out_first = IN_FIRST + nc - PAIR + OUT_OFF

    def prow(w, s, lo=0, count=None):
        return pbuf.at[w, pl.ds(pl.multiple_of(s * rows + lo, half), rows if count is None else count)]

    def rs_copy(w, k, up):
        off = hops - k + 1
        s = chip(off) if up else chip(-off)
        lo, cnt = (0, rows) if k > 1 else ((0, half) if up else (half, half))
        d = 0 if up else 1
        return remote(prow(w, s, lo, cnt), rbuf.at[d, w, k - 1, pl.ds(lo, cnt)], rs_send.at[w], rs_recv.at[d, w, k - 1], nxt if up else prv)

    def push_copy(w):
        return remote(part.at[w % 2], pbuf.at[w], pp_send.at[w % 2], pp_recv.at[w], partner)

    shift = c * nc
    ag_shift = c * AG_SHIFT

    def rs_forward(i):
        for k in range(hops - 1, 0, -1):
            w = i - RS_LAGS[k] - shift

            @pl.when((w >= 0) & (w < nc))
            def _():
                for up in (True, False):
                    rs_copy(w, k, up).wait_recv()
                    d = 0 if up else 1
                    s = chip(hops - k) if up else chip(-(hops - k))
                    lo, cnt = (0, rows) if k > 1 else ((0, half) if up else (half, half))
                    dst = prow(w, s, lo, cnt)
                    dst[...] += rbuf[d, w, k - 1, lo:lo + cnt, :]
                    rs_copy(w, k + 1, up).start()

    def rs_final(i):
        w = i - RS_LAGS[hops] - shift

        @pl.when((w >= 0) & (w < nc))
        def _():
            rs_copy(w, hops, True).wait_recv()
            rs_copy(w, hops, False).wait_recv()
            total = prow(w, z)[...] + (rbuf[0, w, hops - 1] + rbuf[1, w, hops - 1]) + u_all[w]
            y_ref[:, pl.ds(pl.multiple_of(w * COLS, COLS), COLS)] = total.astype(BF16)

    def ag_forward(j):
        for k in range(1, hops):
            w = j - AG_LAGS[k - 1] - ag_shift

            @pl.when((w >= 0) & (w < nc))
            def _():
                for up in (True, False):
                    ag_arrival(w, k, up).wait_recv()
                    ag_copy(w, k + 1, up).start()
                ag_push(w, chip(-k)).start()
                ag_push(w, chip(k)).start()

                @pl.when(w == 0)
                def _():
                    for up in (True, False):
                        tab_copy(k, up, True).wait_recv()
                        tab_copy(k + 1, up, False).start()
                    tab_push(chip(-k)).start()
                    tab_push(chip(k)).start()

        w = j + LEAD - ag_shift

        @pl.when((w >= (1 - c) * LEAD) & (w < nc))
        def _():
            ag_own(w)

        w = j - ag_span - ag_shift

        @pl.when((w >= 0) & (w < nc))
        def _():
            for up in (True, False):
                ag_arrival(w, hops, up).wait_recv()
            ag_push(w, chip(hops)).start()

            @pl.when(w == 0)
            def _():
                for up in (True, False):
                    tab_copy(hops, up, True).wait_recv()
                tab_push(chip(hops)).start()

    def shared_part(j):
        v = j + SI_EARLY

        @pl.when(v < nc)
        def _():
            shared_in(v)

        @pl.when(v == nc)
        def _():
            s_act[...] = gelu(sacc[...]).astype(BF16)

        @pl.when(j == WI_AT)
        def _():
            wi_copy(1).start()

        @pl.when(j == SO_AT - 2)
        def _():
            for q in range(2):
                so_copy(q).start()

        @pl.when(j == WO_AT)
        def _():
            for q in range(2):
                wo_copy(q).start()

        v2 = j - SO_AT

        @pl.when((v2 >= 0) & (v2 < nc))
        def _():
            so_copy(v2).wait()
            u_all[v2] = jnp.dot(s_act[...], so_buf[v2 % 2], preferred_element_type=F32)

            @pl.when(v2 + 2 < nc)
            def _():
                so_copy(v2 + 2).start()

    def in_part(j):
        p = (j - IN_FIRST) // PAIR

        @pl.when((j >= IN_FIRST) & ((j - IN_FIRST) % PAIR == 0) & (p < 2 * pairs_in))
        def _():
            g, m = p // pairs_in, p % pairs_in

            @pl.when(m == 0)
            def _():
                @pl.when(g != c)
                def _():
                    theirs = tabs.at[pl.ds((1 - c) * chips, chips)]
                    pltpu.make_async_copy(theirs, theirs, tab_part).wait()

                build_tables(g)

            @pl.when(g != c)
            def _():
                for q in range(PAIR):
                    v = m * PAIR + q
                    theirs = x_all.at[v, pl.ds(pl.multiple_of((1 - c) * group_rows, group_rows), group_rows)]
                    pltpu.make_async_copy(theirs, theirs, ag_part.at[v]).wait()

            for q in range(PAIR):
                gather(m * PAIR + q, g, q)
            wi_copy(p).wait()

            @pl.when(m == 0)
            def _():
                for e in range(experts):
                    hacc[e] = jnp.dot(xg[e], wi_buf[p % 2, e], preferred_element_type=F32)

            @pl.when((m > 0) & (m < pairs_in - 1))
            def _():
                for e in range(experts):
                    hacc[e] += jnp.dot(xg[e], wi_buf[p % 2, e], preferred_element_type=F32)

            @pl.when((m > 0) & (m == pairs_in - 1))
            def _():
                for e in range(experts):
                    h[g, e] = gelu(hacc[e] + jnp.dot(xg[e], wi_buf[p % 2, e], preferred_element_type=F32)).astype(BF16)

            @pl.when(p + 2 < 2 * pairs_in)
            def _():
                wi_copy(p + 2).start()

    def out_part(i):
        @pl.when((i >= 0) & (i < 2 * nc))
        def _():
            g, w = i // nc, i % nc
            wo_copy(i).wait()
            for e in range(experts):
                outs[e * slots:(e + 1) * slots, :] = jnp.dot(h[g, e], wo_buf[i % 2, e], preferred_element_type=F32).astype(BF16)

            @pl.when((i - 2 >= nc - shift) & (i - 2 < 2 * nc - shift))
            def _():
                push_copy(w).wait_send()

            part[w % 2] = jnp.dot(gate_mat[g], outs[...], preferred_element_type=F32)

            @pl.when(g != c)
            def _():
                push_copy(w).start()

            @pl.when(i + 2 < 2 * nc)
            def _():
                wo_copy(i + 2).start()

    def out_send(i):
        w = i - RS_LAGS[0] - shift

        @pl.when((w >= 0) & (w < nc))
        def _():
            push_copy(w).wait_recv()
            pbuf[w] += part[w % 2]
            rs_copy(w, 1, True).start()
            rs_copy(w, 1, False).start()

    def tick(j, carry):
        i = j - out_first
        ag_forward(j)
        shared_part(j)
        in_part(j)
        rs_forward(i)
        out_part(i)
        out_send(i)
        rs_final(i)
        return carry

    lax.fori_loop(0, out_first + 2 * nc + RS_LAGS[hops], tick, 0)

    def drain(w, carry):
        sent = x_all.at[w, pl.ds(0, (2 * chips - 1) * rows)]
        pltpu.make_async_copy(sent, sent, ag_send.at[w]).wait()
        sums = pbuf.at[w, pl.ds(0, (chips - 1) * rows)]
        pltpu.make_async_copy(sums, sums, rs_send.at[w]).wait()
        return carry

    lax.fori_loop(0, nc, drain, 0)
    sent = tabs.at[pl.ds(0, 2 * chips - 1)]
    pltpu.make_async_copy(sent, sent, tab_send).wait()

    @pl.when(c == 0)
    def _():
        for w in range(2):
            push_copy(w).wait_send()


def solution(mesh):
    group_size = mesh.shape['ep']
    chips = group_size // CORES
    hops = chips // 2

    def local_layer(x_loc, idx_loc, gate_loc, w_in, w_out, shared_in, shared_out):
        rows, top_k = idx_loc.shape
        d_model = x_loc.shape[1]
        experts, _, ff = w_in.shape
        fs = shared_in.shape[1]
        num_experts = experts * group_size
        cap = min(rows, LOAD_MULT * rows * top_k // num_experts)
        slots = chips * cap
        nc = d_model // COLS
        any_spec = pl.BlockSpec(memory_space=pl.ANY)
        dma = pltpu.SemaphoreType.DMA
        flops = 2 * group_size * cap * experts * d_model * ff * 2
        return pl.pallas_call(
            functools.partial(moe_kernel, chips, cap, top_k),
            out_shape=jax.ShapeDtypeStruct((rows, d_model), BF16),
            in_specs=[any_spec] * 7,
            out_specs=pl.BlockSpec(memory_space=pltpu.VMEM),
            scratch_shapes=[
                pltpu.VMEM((nc, group_size * rows, COLS), BF16),
                pltpu.VMEM((top_k, rows), jnp.int32),
                pltpu.VMEM((top_k, rows), F32),
                pltpu.VMEM((group_size, 16, 2 * rows), F32),
                pltpu.VMEM((hops * experts, 2 * rows), F32),
                pltpu.VMEM((2 * experts, chips * rows), F32),
                pltpu.VMEM((2, experts * slots, chips * rows), BF16),
                pltpu.VMEM((2, chips * rows, experts * slots), BF16),
                pltpu.VMEM((experts, slots, PAIR * COLS), BF16),
                pltpu.VMEM((experts, slots, ff), F32),
                pltpu.VMEM((2, experts, slots, ff), BF16),
                pltpu.VMEM((experts * slots, COLS), BF16),
                pltpu.VMEM((nc, chips * rows, COLS), F32),
                pltpu.VMEM((2, chips * rows, COLS), F32),
                pltpu.VMEM((2, nc, hops, rows, COLS), F32),
                pltpu.VMEM((rows, fs), F32),
                pltpu.VMEM((rows, fs), BF16),
                pltpu.VMEM((nc, rows, COLS), F32),
                pltpu.VMEM((2, experts, PAIR * COLS, ff), BF16),
                pltpu.VMEM((2, experts, ff, COLS), BF16),
                pltpu.VMEM((SI_SLOTS, COLS, fs), BF16),
                pltpu.VMEM((2, fs, COLS), BF16),
                dma((2, nc, hops)), dma((2, hops)), dma((nc,)), dma(()), dma((nc,)), dma(()), dma((3,)),
                dma((2, nc, hops)), dma((nc,)), dma((2,)), dma((nc,)),
                dma((2,)), dma((2,)), dma((SI_SLOTS,)), dma((2,)),
            ],
            compiler_params=pltpu.CompilerParams(collective_id=0, has_side_effects=True, vmem_limit_bytes=VMEM_BYTES),
            cost_estimate=pl.CostEstimate(flops=flops, bytes_accessed=2 * (w_in.size + w_out.size + shared_in.size + shared_out.size), transcendentals=0),
        )(x_loc, idx_loc.T, gate_loc.T, w_in, w_out, shared_in, shared_out)

    tok_spec = P(('dp', 'ep'), None)
    expert_spec = P('ep', None, None)
    whole_spec = P(None, None)
    return jax.shard_map(local_layer, mesh=mesh, in_specs=(tok_spec, tok_spec, tok_spec, expert_spec, expert_spec, whole_spec, whole_spec), out_specs=tok_spec, check_vma=False)
```

```python
import functools

import jax
import jax.numpy as jnp
from jax import lax
from jax.experimental import pallas as pl
from jax.experimental.pallas import tpu as pltpu
from jax.sharding import PartitionSpec as P

LOAD_MULT = 3
COLS = 256
LEAD = 8
AG_LAGS = (0, 5, 10, 14)
AG_SHIFT = 12
RS_LAGS = (0, 3, 5, 9, 13)
PAIR = 2
IN_FIRST = 17
OUT_OFF = 0
SI_SLOTS = 4
WO_SLOTS = 3
SI_EARLY = 4
WI_AT, SO_AT, WO_AT = 3, 6, 14
CORES = 2
ABSENT = -4096.0
VMEM_BYTES = 65_000_000
F32 = jnp.float32
BF16 = jnp.bfloat16


def gelu(z):
    return 0.5 * z * (1.0 + jnp.tanh(0.7978845608028654 * (z + 0.044715 * (z * z * z))))


def moe_kernel(chips, cap, top_k,
               x_hbm, idx_hbm, top_hbm, wi_hbm, wo_hbm, si_hbm, so_hbm, y_ref,
               x_all, idx_v, top_v, tabs, picks, codes, pick_mat, gate_mat, xg, hacc, h, outs, pbuf, part, rbuf,
               sacc, s_act, u_all, wi_buf, wo_buf, si_buf, so_buf,
               ag_recv, tab_recv, ag_part, tab_part, ag_send, tab_send, own_sem,
               rs_recv, rs_send, pp_send, pp_recv, wi_sem, wo_sem, si_sem, so_sem):
    rows, d_model = x_hbm.shape
    experts = wi_hbm.shape[0]
    nc = d_model // COLS
    hops = chips // 2
    pairs_in = nc // PAIR
    half = rows // 2
    group_rows = chips * rows
    slots = chips * cap

    ep = lax.axis_index('ep')
    z, c = ep // CORES, ep % CORES
    first = lax.axis_index('dp') * (chips * CORES)
    partner = first + z * CORES + (1 - c)
    nxt = first + ((z + 1) % chips) * CORES + c
    prv = first + ((z + chips - 1) % chips) * CORES + c
    near = [(z + off) % chips for off in range(chips)]

    def chip(off):
        return near[off % chips]

    def xrows(w, s, lo=0, count=None):
        base = (c * chips + s) * rows + lo
        return x_all.at[w, pl.ds(pl.multiple_of(base, half), rows if count is None else count)]

    def tblk(s, lo=0, count=None):
        t = tabs.at[c * chips + s]
        return t if count is None else t.at[pl.ds(lo, count)]

    def remote(src, dst, ssem, rsem, dev):
        return pltpu.make_async_remote_copy(src_ref=src, dst_ref=dst, send_sem=ssem, recv_sem=rsem, device_id=dev, device_id_type=pl.DeviceIdType.LOGICAL)

    def ag_copy(w, k, up):
        s = chip(-(k - 1)) if up else chip(k - 1)
        lo, cnt = (0, None) if k < hops else ((0, half) if up else (half, half))
        ref = xrows(w, s, lo, cnt)
        return remote(ref, ref, ag_send.at[w], ag_recv.at[0 if up else 1, w, k - 1], nxt if up else prv)

    def ag_arrival(w, k, up):
        s = chip(-k) if up else chip(k)
        lo, cnt = (0, None) if k < hops else ((0, half) if up else (half, half))
        ref = xrows(w, s, lo, cnt)
        return remote(ref, ref, ag_send.at[w], ag_recv.at[0 if up else 1, w, k - 1], nxt if up else prv)

    def tab_copy(k, up, arrival):
        off = k if arrival else k - 1
        s = chip(-off) if up else chip(off)
        lo, cnt = (0, None) if k < hops else ((0, 8) if up else (8, 8))
        ref = tblk(s, lo, cnt)
        return remote(ref, ref, tab_send, tab_recv.at[0 if up else 1, k - 1], nxt if up else prv)

    def ag_push(w, s):
        ref = xrows(w, s)
        return remote(ref, ref, ag_send.at[w], ag_part.at[w], partner)

    def tab_push(s):
        ref = tblk(s)
        return remote(ref, ref, tab_send, tab_part, partner)

    def wi_copy(w):
        return pltpu.make_async_copy(wi_hbm.at[:, pl.ds(pl.multiple_of(w % pairs_in * (PAIR * COLS), COLS), PAIR * COLS), :], wi_buf.at[w % 2], wi_sem.at[w % 2])

    def wo_copy(w):
        return pltpu.make_async_copy(wo_hbm.at[:, :, pl.ds(pl.multiple_of(w % nc * COLS, COLS), COLS)], wo_buf.at[w % WO_SLOTS], wo_sem.at[w % WO_SLOTS])

    def si_copy(w):
        return pltpu.make_async_copy(si_hbm.at[pl.ds(pl.multiple_of(w * COLS, COLS), COLS), :], si_buf.at[w % SI_SLOTS], si_sem.at[w % SI_SLOTS])

    def so_copy(w):
        return pltpu.make_async_copy(so_hbm.at[:, pl.ds(pl.multiple_of(w * COLS, COLS), COLS)], so_buf.at[w % 2], so_sem.at[w % 2])

    for w in range(nc):
        pltpu.make_async_copy(x_hbm.at[:, pl.ds(w * COLS, COLS)], xrows(w, z), own_sem.at[0]).start()
    pltpu.make_async_copy(idx_hbm, idx_v, own_sem.at[1]).start()
    pltpu.make_async_copy(top_hbm, top_v, own_sem.at[2]).start()
    for w in range(min(SI_SLOTS, nc)):
        si_copy(w).start()

    barrier = pltpu.get_barrier_semaphore()
    for dev in (nxt, prv, partner):
        pl.semaphore_signal(barrier, inc=1, device_id=dev, device_id_type=pl.DeviceIdType.LOGICAL)
    pl.semaphore_wait(barrier, 3)

    pltpu.make_async_copy(idx_hbm, idx_v, own_sem.at[1]).wait()
    pltpu.make_async_copy(top_hbm, top_v, own_sem.at[2]).wait()
    right = lax.broadcasted_iota(jnp.int32, (top_k, 2 * rows), 1) >= rows
    side = right == (z % 2 == 1)
    ids, gts = idx_v[...].astype(F32), top_v[...]
    mine = tabs.at[c * chips + z]
    mine[...] = jnp.zeros_like(mine)
    mine[0:top_k, :] = jnp.where(side, jnp.concatenate([ids, ids], axis=1), 0.0)
    mine[8:8 + top_k, :] = jnp.where(side, jnp.concatenate([gts, gts], axis=1), 0.0)
    own_all = x_all.at[0, pl.ds(0, nc * rows)]
    pltpu.make_async_copy(own_all, own_all, own_sem.at[0]).wait()
    def ag_own(w):
        ag_copy(w, 1, True).start()
        ag_copy(w, 1, False).start()
        ag_push(w, z).start()

    @pl.when(c == 0)
    def _():
        for w in range(min(LEAD, nc)):
            ag_own(w)

    tab_copy(1, True, False).start()
    tab_copy(1, False, False).start()
    tab_push(z).start()

    def shared_in(v):
        si_copy(v).wait()
        own = x_all[v, pl.ds(pl.multiple_of((c * chips + z) * rows, rows), rows), :]
        sacc[...] += jnp.dot(own, si_buf[v % SI_SLOTS], preferred_element_type=F32)

        @pl.when(v + SI_SLOTS < nc)
        def _():
            si_copy(v + SI_SLOTS).start()

    sacc[...] = jnp.zeros_like(sacc)

    def early_step(v, carry):
        shared_in(v)
        return carry

    lax.fori_loop(0, SI_EARLY, early_step, 0)
    wi_copy(0).start()

    def build_tables(g):
        base = (ep * experts).astype(F32)
        lane = lax.broadcasted_iota(jnp.int32, (1, 2 * rows), 1)
        pairs = chips // 2
        for i in range(pairs):
            t = tabs[g * chips + 2 * i] + tabs[g * chips + 2 * i + 1]
            ids, gts = t[0:top_k], t[8:8 + top_k]
            for e in range(experts):
                hit = ids == (base + float(e))
                r = i * experts + e
                picks[r:r + 1, :] = jnp.sum(hit.astype(F32), axis=0, keepdims=True)
                codes[experts + e:experts + e + 1, i * 2 * rows:(i + 1) * 2 * rows] = jnp.sum(jnp.where(hit, gts, 0.0), axis=0, keepdims=True)
        a = lax.broadcasted_iota(jnp.int32, (2 * rows, 2 * rows), 0)
        b = lax.broadcasted_iota(jnp.int32, (2 * rows, 2 * rows), 1)
        before = ((a < b) & ((a >= rows) == (b >= rows))).astype(F32).astype(BF16)
        rank = jnp.dot(picks[...].astype(BF16), before, preferred_element_type=F32)
        for i in range(pairs):
            start = (2 * i * cap + jnp.where(lane >= rows, cap, 0)).astype(F32)
            for e in range(experts):
                r = i * experts + e
                code = jnp.where(picks[r:r + 1, :] > 0.5, rank[r:r + 1, :] + start, ABSENT)
                codes[e:e + 1, i * 2 * rows:(i + 1) * 2 * rows] = code
        slot = lax.broadcasted_iota(jnp.int32, (slots, group_rows), 0).astype(F32)
        col = lax.broadcasted_iota(jnp.int32, (2 * rows, experts * slots), 1).astype(F32)
        for e in range(experts):
            pick_mat[g, e * slots:(e + 1) * slots, :] = jnp.where(slot == codes[e:e + 1, :], 1.0, 0.0).astype(BF16)
        for i in range(pairs):
            ct = jnp.transpose(codes[:, i * 2 * rows:(i + 1) * 2 * rows])
            acc = jnp.zeros((2 * rows, experts * slots), F32)
            for e in range(experts):
                acc = jnp.where(col == ct[:, e:e + 1] + float(e * slots), ct[:, experts + e:experts + e + 1], acc)
            gate_mat[g, i * 2 * rows:(i + 1) * 2 * rows, :] = acc.astype(BF16)

    def gather(w, g, q):
        xs = x_all[w, pl.ds(pl.multiple_of(g * group_rows, group_rows), group_rows), :]
        got = jnp.dot(pick_mat[g], xs, preferred_element_type=F32).astype(BF16)
        for e in range(experts):
            xg[e, :, q * COLS:(q + 1) * COLS] = got[e * slots:(e + 1) * slots, :]

    ag_span = AG_LAGS[hops - 1]
    out_first = IN_FIRST + nc - PAIR + OUT_OFF

    def prow(w, s, lo=0, count=None):
        return pbuf.at[w, pl.ds(pl.multiple_of(s * rows + lo, half), rows if count is None else count)]

    def rs_copy(w, k, up):
        off = hops - k + 1
        s = chip(off) if up else chip(-off)
        lo, cnt = (0, rows) if k > 1 else ((0, half) if up else (half, half))
        d = 0 if up else 1
        return remote(prow(w, s, lo, cnt), rbuf.at[d, w, k - 1, pl.ds(lo, cnt)], rs_send.at[w], rs_recv.at[d, w, k - 1], nxt if up else prv)

    def push_copy(w):
        return remote(part.at[w % 2], pbuf.at[w], pp_send.at[w % 2], pp_recv.at[w], partner)

    shift = c * nc
    ag_shift = c * AG_SHIFT

    def rs_forward(i):
        for k in range(1, hops):
            w = i - RS_LAGS[k] - shift

            @pl.when((w >= 0) & (w < nc))
            def _():
                for up in (True, False):
                    rs_copy(w, k, up).wait_recv()
                    d = 0 if up else 1
                    s = chip(hops - k) if up else chip(-(hops - k))
                    lo, cnt = (0, rows) if k > 1 else ((0, half) if up else (half, half))
                    dst = prow(w, s, lo, cnt)
                    dst[...] += rbuf[d, w, k - 1, lo:lo + cnt, :]
                    rs_copy(w, k + 1, up).start()

    def rs_final(i):
        w = i - RS_LAGS[hops] - shift

        @pl.when((w >= 0) & (w < nc))
        def _():
            rs_copy(w, hops, True).wait_recv()
            rs_copy(w, hops, False).wait_recv()
            total = prow(w, z)[...] + (rbuf[0, w, hops - 1] + rbuf[1, w, hops - 1]) + u_all[w]
            y_ref[:, pl.ds(pl.multiple_of(w * COLS, COLS), COLS)] = total.astype(BF16)

    def ag_forward(j):
        for k in range(hops - 1, 0, -1):
            w = j - AG_LAGS[k - 1] - ag_shift

            @pl.when((w >= 0) & (w < nc))
            def _():
                for up in (True, False):
                    ag_arrival(w, k, up).wait_recv()
                    ag_copy(w, k + 1, up).start()
                ag_push(w, chip(-k)).start()
                ag_push(w, chip(k)).start()

                @pl.when(w == 0)
                def _():
                    for up in (True, False):
                        tab_copy(k, up, True).wait_recv()
                        tab_copy(k + 1, up, False).start()
                    tab_push(chip(-k)).start()
                    tab_push(chip(k)).start()

        w = j + LEAD - ag_shift

        @pl.when((w >= (1 - c) * LEAD) & (w < nc))
        def _():
            ag_own(w)

        w = j - ag_span - ag_shift

        @pl.when((w >= 0) & (w < nc))
        def _():
            for up in (True, False):
                ag_arrival(w, hops, up).wait_recv()
            ag_push(w, chip(hops)).start()

            @pl.when(w == 0)
            def _():
                for up in (True, False):
                    tab_copy(hops, up, True).wait_recv()
                tab_push(chip(hops)).start()

    def shared_part(j):
        v = j + SI_EARLY

        @pl.when(v < nc)
        def _():
            shared_in(v)

        @pl.when(v == nc)
        def _():
            s_act[...] = gelu(sacc[...]).astype(BF16)

        @pl.when(j == WI_AT)
        def _():
            wi_copy(1).start()

        @pl.when(j == SO_AT - 2)
        def _():
            for q in range(2):
                so_copy(q).start()

        @pl.when(j == WO_AT)
        def _():
            for q in range(WO_SLOTS):
                wo_copy(q).start()

        v2 = j - SO_AT

        @pl.when((v2 >= 0) & (v2 < nc))
        def _():
            so_copy(v2).wait()
            u_all[v2] = jnp.dot(s_act[...], so_buf[v2 % 2], preferred_element_type=F32)

            @pl.when(v2 + 2 < nc)
            def _():
                so_copy(v2 + 2).start()

    def in_part(j):
        p = (j - IN_FIRST) // PAIR

        @pl.when((j >= IN_FIRST) & ((j - IN_FIRST) % PAIR == 0) & (p < 2 * pairs_in))
        def _():
            g, m = p // pairs_in, p % pairs_in

            @pl.when(m == 0)
            def _():
                @pl.when(g != c)
                def _():
                    theirs = tabs.at[pl.ds((1 - c) * chips, chips)]
                    pltpu.make_async_copy(theirs, theirs, tab_part).wait()

                build_tables(g)

            @pl.when(g != c)
            def _():
                for q in range(PAIR):
                    v = m * PAIR + q
                    theirs = x_all.at[v, pl.ds(pl.multiple_of((1 - c) * group_rows, group_rows), group_rows)]
                    pltpu.make_async_copy(theirs, theirs, ag_part.at[v]).wait()

            for q in range(PAIR):
                gather(m * PAIR + q, g, q)
            wi_copy(p).wait()

            @pl.when(m == 0)
            def _():
                for e in range(experts):
                    hacc[e] = jnp.dot(xg[e], wi_buf[p % 2, e], preferred_element_type=F32)

            @pl.when((m > 0) & (m < pairs_in - 1))
            def _():
                for e in range(experts):
                    hacc[e] += jnp.dot(xg[e], wi_buf[p % 2, e], preferred_element_type=F32)

            @pl.when((m > 0) & (m == pairs_in - 1))
            def _():
                for e in range(experts):
                    h[g, e] = gelu(hacc[e] + jnp.dot(xg[e], wi_buf[p % 2, e], preferred_element_type=F32)).astype(BF16)

            @pl.when(p + 2 < 2 * pairs_in)
            def _():
                wi_copy(p + 2).start()

    def out_part(i):
        @pl.when((i >= 0) & (i < 2 * nc))
        def _():
            g, w = i // nc, i % nc
            wo_copy(i).wait()
            for e in range(experts):
                outs[e * slots:(e + 1) * slots, :] = jnp.dot(h[g, e], wo_buf[i % WO_SLOTS, e], preferred_element_type=F32).astype(BF16)

            @pl.when((i - 2 >= nc - shift) & (i - 2 < 2 * nc - shift))
            def _():
                push_copy(w).wait_send()

            part[w % 2] = jnp.dot(gate_mat[g], outs[...], preferred_element_type=F32)

            @pl.when(g != c)
            def _():
                push_copy(w).start()

            @pl.when(i + WO_SLOTS < 2 * nc)
            def _():
                wo_copy(i + WO_SLOTS).start()

    def out_send(i):
        w = i - RS_LAGS[0] - shift

        @pl.when((w >= 0) & (w < nc))
        def _():
            push_copy(w).wait_recv()
            pbuf[w] += part[w % 2]
            rs_copy(w, 1, True).start()
            rs_copy(w, 1, False).start()

    def tick(j, carry):
        i = j - out_first
        ag_forward(j)
        shared_part(j)
        rs_forward(i)
        in_part(j)
        out_part(i)
        out_send(i)
        rs_final(i)
        return carry

    lax.fori_loop(0, out_first + 2 * nc + RS_LAGS[hops], tick, 0)

    def drain(w, carry):
        sent = x_all.at[w, pl.ds(0, (2 * chips - 1) * rows)]
        pltpu.make_async_copy(sent, sent, ag_send.at[w]).wait()
        sums = pbuf.at[w, pl.ds(0, (chips - 1) * rows)]
        pltpu.make_async_copy(sums, sums, rs_send.at[w]).wait()
        return carry

    lax.fori_loop(0, nc, drain, 0)
    sent = tabs.at[pl.ds(0, 2 * chips - 1)]
    pltpu.make_async_copy(sent, sent, tab_send).wait()

    @pl.when(c == 0)
    def _():
        for w in range(2):
            push_copy(w).wait_send()


def solution(mesh):
    group_size = mesh.shape['ep']
    chips = group_size // CORES
    hops = chips // 2

    def local_layer(x_loc, idx_loc, gate_loc, w_in, w_out, shared_in, shared_out):
        rows, top_k = idx_loc.shape
        d_model = x_loc.shape[1]
        experts, _, ff = w_in.shape
        fs = shared_in.shape[1]
        num_experts = experts * group_size
        cap = min(rows, LOAD_MULT * rows * top_k // num_experts)
        slots = chips * cap
        nc = d_model // COLS
        any_spec = pl.BlockSpec(memory_space=pl.ANY)
        dma = pltpu.SemaphoreType.DMA
        flops = 2 * group_size * cap * experts * d_model * ff * 2
        return pl.pallas_call(
            functools.partial(moe_kernel, chips, cap, top_k),
            out_shape=pltpu.VMEM((rows, d_model), BF16),
            in_specs=[any_spec] * 7,
            out_specs=pl.BlockSpec(memory_space=pltpu.VMEM),
            scratch_shapes=[
                pltpu.VMEM((nc, group_size * rows, COLS), BF16),
                pltpu.VMEM((top_k, rows), jnp.int32),
                pltpu.VMEM((top_k, rows), F32),
                pltpu.VMEM((group_size, 16, 2 * rows), F32),
                pltpu.VMEM((hops * experts, 2 * rows), F32),
                pltpu.VMEM((2 * experts, chips * rows), F32),
                pltpu.VMEM((2, experts * slots, chips * rows), BF16),
                pltpu.VMEM((2, chips * rows, experts * slots), BF16),
                pltpu.VMEM((experts, slots, PAIR * COLS), BF16),
                pltpu.VMEM((experts, slots, ff), F32),
                pltpu.VMEM((2, experts, slots, ff), BF16),
                pltpu.VMEM((experts * slots, COLS), BF16),
                pltpu.VMEM((nc, chips * rows, COLS), F32),
                pltpu.VMEM((2, chips * rows, COLS), F32),
                pltpu.VMEM((2, nc, hops, rows, COLS), F32),
                pltpu.VMEM((rows, fs), F32),
                pltpu.VMEM((rows, fs), BF16),
                pltpu.VMEM((nc, rows, COLS), F32),
                pltpu.VMEM((2, experts, PAIR * COLS, ff), BF16),
                pltpu.VMEM((WO_SLOTS, experts, ff, COLS), BF16),
                pltpu.VMEM((SI_SLOTS, COLS, fs), BF16),
                pltpu.VMEM((2, fs, COLS), BF16),
                dma((2, nc, hops)), dma((2, hops)), dma((nc,)), dma(()), dma((nc,)), dma(()), dma((3,)),
                dma((2, nc, hops)), dma((nc,)), dma((2,)), dma((nc,)),
                dma((2,)), dma((WO_SLOTS,)), dma((SI_SLOTS,)), dma((2,)),
            ],
            compiler_params=pltpu.CompilerParams(collective_id=0, has_side_effects=True, vmem_limit_bytes=VMEM_BYTES),
            cost_estimate=pl.CostEstimate(flops=flops, bytes_accessed=2 * (w_in.size + w_out.size + shared_in.size + shared_out.size), transcendentals=0),
        )(x_loc, idx_loc.T, gate_loc.T, w_in, w_out, shared_in, shared_out)

    tok_spec = P(('dp', 'ep'), None)
    expert_spec = P('ep', None, None)
    whole_spec = P(None, None)
    return jax.shard_map(local_layer, mesh=mesh, in_specs=(tok_spec, tok_spec, tok_spec, expert_spec, expert_spec, whole_spec, whole_spec), out_specs=tok_spec, check_vma=False)
```

```python
import functools

import jax
import jax.numpy as jnp
from jax import lax
from jax.experimental import pallas as pl
from jax.experimental.pallas import tpu as pltpu
from jax.sharding import PartitionSpec as P

LOAD_MULT = 3
COLS = 256
LEAD = 6
AG_LAGS = (0, 4, 8, 11)
AG_SHIFT = 13
RS_LAGS = (0, 3, 5, 9, 13)
PAIR = 2
IN_FIRST = 15
OUT_OFF = 0
SI_SLOTS = 4
WO_SLOTS = 3
SI_EARLY = 4
WI_AT, SO_AT, WO_AT = 3, 6, 14
CORES = 2
ABSENT = -4096.0
VMEM_BYTES = 65_000_000
F32 = jnp.float32
BF16 = jnp.bfloat16


def gelu(z):
    return 0.5 * z * (1.0 + jnp.tanh(0.7978845608028654 * (z + 0.044715 * (z * z * z))))


def moe_kernel(chips, cap, top_k,
               x_hbm, idx_hbm, top_hbm, wi_hbm, wo_hbm, si_hbm, so_hbm, y_ref,
               x_all, idx_v, top_v, tabs, picks, codes, pick_mat, gate_mat, xg, hacc, h, outs, pbuf, part, rbuf,
               sacc, s_act, u_all, wi_buf, wo_buf, si_buf, so_buf,
               ag_recv, tab_recv, ag_part, tab_part, ag_send, tab_send, own_sem,
               rs_recv, rs_send, pp_send, pp_recv, wi_sem, wo_sem, si_sem, so_sem):
    rows, d_model = x_hbm.shape
    experts = wi_hbm.shape[0]
    nc = d_model // COLS
    hops = chips // 2
    pairs_in = nc // PAIR
    half = rows // 2
    group_rows = chips * rows
    slots = chips * cap

    ep = lax.axis_index('ep')
    z, c = ep // CORES, ep % CORES
    first = lax.axis_index('dp') * (chips * CORES)
    partner = first + z * CORES + (1 - c)
    nxt = first + ((z + 1) % chips) * CORES + c
    prv = first + ((z + chips - 1) % chips) * CORES + c
    near = [(z + off) % chips for off in range(chips)]

    def chip(off):
        return near[off % chips]

    def xrows(w, s, lo=0, count=None):
        base = (c * chips + s) * rows + lo
        return x_all.at[w, pl.ds(pl.multiple_of(base, half), rows if count is None else count)]

    def tblk(s, lo=0, count=None):
        t = tabs.at[c * chips + s]
        return t if count is None else t.at[pl.ds(lo, count)]

    def remote(src, dst, ssem, rsem, dev):
        return pltpu.make_async_remote_copy(src_ref=src, dst_ref=dst, send_sem=ssem, recv_sem=rsem, device_id=dev, device_id_type=pl.DeviceIdType.LOGICAL)

    def ag_copy(w, k, up):
        s = chip(-(k - 1)) if up else chip(k - 1)
        lo, cnt = (0, None) if k < hops else ((0, half) if up else (half, half))
        ref = xrows(w, s, lo, cnt)
        return remote(ref, ref, ag_send.at[w], ag_recv.at[0 if up else 1, w, k - 1], nxt if up else prv)

    def ag_arrival(w, k, up):
        s = chip(-k) if up else chip(k)
        lo, cnt = (0, None) if k < hops else ((0, half) if up else (half, half))
        ref = xrows(w, s, lo, cnt)
        return remote(ref, ref, ag_send.at[w], ag_recv.at[0 if up else 1, w, k - 1], nxt if up else prv)

    def tab_copy(k, up, arrival):
        off = k if arrival else k - 1
        s = chip(-off) if up else chip(off)
        lo, cnt = (0, None) if k < hops else ((0, 8) if up else (8, 8))
        ref = tblk(s, lo, cnt)
        return remote(ref, ref, tab_send, tab_recv.at[0 if up else 1, k - 1], nxt if up else prv)

    def ag_push(w, s):
        ref = xrows(w, s)
        return remote(ref, ref, ag_send.at[w], ag_part.at[w], partner)

    def tab_push(s):
        ref = tblk(s)
        return remote(ref, ref, tab_send, tab_part, partner)

    def wi_copy(w):
        return pltpu.make_async_copy(wi_hbm.at[:, pl.ds(pl.multiple_of(w % pairs_in * (PAIR * COLS), COLS), PAIR * COLS), :], wi_buf.at[w % 2], wi_sem.at[w % 2])

    def wo_copy(w):
        return pltpu.make_async_copy(wo_hbm.at[:, :, pl.ds(pl.multiple_of(w % nc * COLS, COLS), COLS)], wo_buf.at[w % WO_SLOTS], wo_sem.at[w % WO_SLOTS])

    def si_copy(w):
        return pltpu.make_async_copy(si_hbm.at[pl.ds(pl.multiple_of(w * COLS, COLS), COLS), :], si_buf.at[w % SI_SLOTS], si_sem.at[w % SI_SLOTS])

    def so_copy(w):
        return pltpu.make_async_copy(so_hbm.at[:, pl.ds(pl.multiple_of(w * COLS, COLS), COLS)], so_buf.at[w % 2], so_sem.at[w % 2])

    for w in range(nc):
        pltpu.make_async_copy(x_hbm.at[:, pl.ds(w * COLS, COLS)], xrows(w, z), own_sem.at[0]).start()
    pltpu.make_async_copy(idx_hbm, idx_v, own_sem.at[1]).start()
    pltpu.make_async_copy(top_hbm, top_v, own_sem.at[2]).start()
    for w in range(min(SI_SLOTS, nc)):
        si_copy(w).start()

    barrier = pltpu.get_barrier_semaphore()
    for dev in (nxt, prv, partner):
        pl.semaphore_signal(barrier, inc=1, device_id=dev, device_id_type=pl.DeviceIdType.LOGICAL)
    pl.semaphore_wait(barrier, 3)

    pltpu.make_async_copy(idx_hbm, idx_v, own_sem.at[1]).wait()
    pltpu.make_async_copy(top_hbm, top_v, own_sem.at[2]).wait()
    right = lax.broadcasted_iota(jnp.int32, (top_k, 2 * rows), 1) >= rows
    side = right == (z % 2 == 1)
    ids, gts = idx_v[...].astype(F32), top_v[...]
    mine = tabs.at[c * chips + z]
    mine[...] = jnp.zeros_like(mine)
    mine[0:top_k, :] = jnp.where(side, jnp.concatenate([ids, ids], axis=1), 0.0)
    mine[8:8 + top_k, :] = jnp.where(side, jnp.concatenate([gts, gts], axis=1), 0.0)
    own_all = x_all.at[0, pl.ds(0, nc * rows)]
    pltpu.make_async_copy(own_all, own_all, own_sem.at[0]).wait()
    def ag_own(w):
        ag_copy(w, 1, True).start()
        ag_copy(w, 1, False).start()
        ag_push(w, z).start()

    @pl.when(c == 0)
    def _():
        for w in range(min(LEAD, nc)):
            ag_own(w)

    tab_copy(1, True, False).start()
    tab_copy(1, False, False).start()
    tab_push(z).start()

    def shared_in(v):
        si_copy(v).wait()
        own = x_all[v, pl.ds(pl.multiple_of((c * chips + z) * rows, rows), rows), :]
        sacc[...] += jnp.dot(own, si_buf[v % SI_SLOTS], preferred_element_type=F32)

        @pl.when(v + SI_SLOTS < nc)
        def _():
            si_copy(v + SI_SLOTS).start()

    sacc[...] = jnp.zeros_like(sacc)

    def early_step(v, carry):
        shared_in(v)
        return carry

    lax.fori_loop(0, SI_EARLY, early_step, 0)
    wi_copy(0).start()

    def build_tables(g):
        base = (ep * experts).astype(F32)
        lane = lax.broadcasted_iota(jnp.int32, (1, 2 * rows), 1)
        pairs = chips // 2
        for i in range(pairs):
            t = tabs[g * chips + 2 * i] + tabs[g * chips + 2 * i + 1]
            ids, gts = t[0:top_k], t[8:8 + top_k]
            for e in range(experts):
                hit = ids == (base + float(e))
                r = i * experts + e
                picks[r:r + 1, :] = jnp.sum(hit.astype(F32), axis=0, keepdims=True)
                codes[experts + e:experts + e + 1, i * 2 * rows:(i + 1) * 2 * rows] = jnp.sum(jnp.where(hit, gts, 0.0), axis=0, keepdims=True)
        a = lax.broadcasted_iota(jnp.int32, (2 * rows, 2 * rows), 0)
        b = lax.broadcasted_iota(jnp.int32, (2 * rows, 2 * rows), 1)
        before = ((a < b) & ((a >= rows) == (b >= rows))).astype(F32).astype(BF16)
        rank = jnp.dot(picks[...].astype(BF16), before, preferred_element_type=F32)
        for i in range(pairs):
            start = (2 * i * cap + jnp.where(lane >= rows, cap, 0)).astype(F32)
            for e in range(experts):
                r = i * experts + e
                code = jnp.where(picks[r:r + 1, :] > 0.5, rank[r:r + 1, :] + start, ABSENT)
                codes[e:e + 1, i * 2 * rows:(i + 1) * 2 * rows] = code
        slot = lax.broadcasted_iota(jnp.int32, (slots, group_rows), 0).astype(F32)
        col = lax.broadcasted_iota(jnp.int32, (2 * rows, experts * slots), 1).astype(F32)
        for e in range(experts):
            pick_mat[g, e * slots:(e + 1) * slots, :] = jnp.where(slot == codes[e:e + 1, :], 1.0, 0.0).astype(BF16)
        for i in range(pairs):
            ct = jnp.transpose(codes[:, i * 2 * rows:(i + 1) * 2 * rows])
            acc = jnp.zeros((2 * rows, experts * slots), F32)
            for e in range(experts):
                acc = jnp.where(col == ct[:, e:e + 1] + float(e * slots), ct[:, experts + e:experts + e + 1], acc)
            gate_mat[g, i * 2 * rows:(i + 1) * 2 * rows, :] = acc.astype(BF16)

    def gather(w, g, q):
        xs = x_all[w, pl.ds(pl.multiple_of(g * group_rows, group_rows), group_rows), :]
        got = jnp.dot(pick_mat[g], xs, preferred_element_type=F32).astype(BF16)
        for e in range(experts):
            xg[e, :, q * COLS:(q + 1) * COLS] = got[e * slots:(e + 1) * slots, :]

    ag_span = AG_LAGS[hops - 1]
    out_first = IN_FIRST + nc - PAIR + OUT_OFF

    def prow(w, s, lo=0, count=None):
        return pbuf.at[w, pl.ds(pl.multiple_of(s * rows + lo, half), rows if count is None else count)]

    def rs_copy(w, k, up):
        off = hops - k + 1
        s = chip(off) if up else chip(-off)
        lo, cnt = (0, rows) if k > 1 else ((0, half) if up else (half, half))
        d = 0 if up else 1
        return remote(prow(w, s, lo, cnt), rbuf.at[d, w, k - 1, pl.ds(lo, cnt)], rs_send.at[w], rs_recv.at[d, w, k - 1], nxt if up else prv)

    def push_copy(w):
        return remote(part.at[w % 2], pbuf.at[w], pp_send.at[w % 2], pp_recv.at[w], partner)

    shift = c * nc
    ag_shift = c * AG_SHIFT

    def rs_forward(i):
        for k in range(1, hops):
            w = i - RS_LAGS[k] - shift

            @pl.when((w >= 0) & (w < nc))
            def _():
                for up in (True, False):
                    rs_copy(w, k, up).wait_recv()
                    d = 0 if up else 1
                    s = chip(hops - k) if up else chip(-(hops - k))
                    lo, cnt = (0, rows) if k > 1 else ((0, half) if up else (half, half))
                    dst = prow(w, s, lo, cnt)
                    dst[...] += rbuf[d, w, k - 1, lo:lo + cnt, :]
                    rs_copy(w, k + 1, up).start()

    def rs_final(i):
        w = i - RS_LAGS[hops] - shift

        @pl.when((w >= 0) & (w < nc))
        def _():
            rs_copy(w, hops, True).wait_recv()
            rs_copy(w, hops, False).wait_recv()
            total = prow(w, z)[...] + (rbuf[0, w, hops - 1] + rbuf[1, w, hops - 1]) + u_all[w]
            y_ref[:, pl.ds(pl.multiple_of(w * COLS, COLS), COLS)] = total.astype(BF16)

    def ag_forward(j):
        for k in range(hops - 1, 0, -1):
            w = j - AG_LAGS[k - 1] - ag_shift

            @pl.when((w >= 0) & (w < nc))
            def _():
                for up in (True, False):
                    ag_arrival(w, k, up).wait_recv()
                    ag_copy(w, k + 1, up).start()
                ag_push(w, chip(-k)).start()
                ag_push(w, chip(k)).start()

                @pl.when(w == 0)
                def _():
                    for up in (True, False):
                        tab_copy(k, up, True).wait_recv()
                        tab_copy(k + 1, up, False).start()
                    tab_push(chip(-k)).start()
                    tab_push(chip(k)).start()

        w = j + LEAD - ag_shift

        @pl.when((w >= (1 - c) * LEAD) & (w < nc))
        def _():
            ag_own(w)

        w = j - ag_span - ag_shift

        @pl.when((w >= 0) & (w < nc))
        def _():
            for up in (True, False):
                ag_arrival(w, hops, up).wait_recv()
            ag_push(w, chip(hops)).start()

            @pl.when(w == 0)
            def _():
                for up in (True, False):
                    tab_copy(hops, up, True).wait_recv()
                tab_push(chip(hops)).start()

    def shared_part(j):
        v = j + SI_EARLY

        @pl.when(v < nc)
        def _():
            shared_in(v)

        @pl.when(v == nc)
        def _():
            s_act[...] = gelu(sacc[...]).astype(BF16)

        @pl.when(j == WI_AT)
        def _():
            wi_copy(1).start()

        @pl.when(j == SO_AT - 2)
        def _():
            for q in range(2):
                so_copy(q).start()

        @pl.when(j == WO_AT)
        def _():
            for q in range(WO_SLOTS):
                wo_copy(q).start()

        v2 = j - SO_AT

        @pl.when((v2 >= 0) & (v2 < nc))
        def _():
            so_copy(v2).wait()
            u_all[v2] = jnp.dot(s_act[...], so_buf[v2 % 2], preferred_element_type=F32)

            @pl.when(v2 + 2 < nc)
            def _():
                so_copy(v2 + 2).start()

    def table_part(j):
        span = pairs_in * PAIR

        @pl.when((j == IN_FIRST - 1) | (j == IN_FIRST + span))
        def _():
            g = (j - (IN_FIRST - 1)) // span

            @pl.when(g != c)
            def _():
                theirs = tabs.at[pl.ds((1 - c) * chips, chips)]
                pltpu.make_async_copy(theirs, theirs, tab_part).wait()

            build_tables(g)

    def in_part(j):
        p = (j - IN_FIRST) // PAIR

        @pl.when((j >= IN_FIRST) & ((j - IN_FIRST) % PAIR == 0) & (p < 2 * pairs_in))
        def _():
            g, m = p // pairs_in, p % pairs_in

            @pl.when(g != c)
            def _():
                for q in range(PAIR):
                    v = m * PAIR + q
                    theirs = x_all.at[v, pl.ds(pl.multiple_of((1 - c) * group_rows, group_rows), group_rows)]
                    pltpu.make_async_copy(theirs, theirs, ag_part.at[v]).wait()

            for q in range(PAIR):
                gather(m * PAIR + q, g, q)
            wi_copy(p).wait()

            @pl.when(m == 0)
            def _():
                for e in range(experts):
                    hacc[e] = jnp.dot(xg[e], wi_buf[p % 2, e], preferred_element_type=F32)

            @pl.when((m > 0) & (m < pairs_in - 1))
            def _():
                for e in range(experts):
                    hacc[e] += jnp.dot(xg[e], wi_buf[p % 2, e], preferred_element_type=F32)

            @pl.when((m > 0) & (m == pairs_in - 1))
            def _():
                for e in range(experts):
                    h[g, e] = gelu(hacc[e] + jnp.dot(xg[e], wi_buf[p % 2, e], preferred_element_type=F32)).astype(BF16)

            @pl.when(p + 2 < 2 * pairs_in)
            def _():
                wi_copy(p + 2).start()

    def out_part(i):
        @pl.when((i >= 0) & (i < 2 * nc))
        def _():
            g, w = i // nc, i % nc
            wo_copy(i).wait()
            for e in range(experts):
                outs[e * slots:(e + 1) * slots, :] = jnp.dot(h[g, e], wo_buf[i % WO_SLOTS, e], preferred_element_type=F32).astype(BF16)

            @pl.when((i - 2 >= nc - shift) & (i - 2 < 2 * nc - shift))
            def _():
                push_copy(w).wait_send()

            part[w % 2] = jnp.dot(gate_mat[g], outs[...], preferred_element_type=F32)

            @pl.when(g != c)
            def _():
                push_copy(w).start()

            @pl.when(i + WO_SLOTS < 2 * nc)
            def _():
                wo_copy(i + WO_SLOTS).start()

    def out_send(i):
        w = i - RS_LAGS[0] - shift

        @pl.when((w >= 0) & (w < nc))
        def _():
            push_copy(w).wait_recv()
            pbuf[w] += part[w % 2]
            rs_copy(w, 1, True).start()
            rs_copy(w, 1, False).start()

    def tick(j, carry):
        i = j - out_first
        ag_forward(j)
        shared_part(j)
        rs_forward(i)
        table_part(j)
        in_part(j)
        out_part(i)
        out_send(i)
        rs_final(i)
        return carry

    lax.fori_loop(0, out_first + 2 * nc + RS_LAGS[hops], tick, 0)

    def drain(w, carry):
        sent = x_all.at[w, pl.ds(0, (2 * chips - 1) * rows)]
        pltpu.make_async_copy(sent, sent, ag_send.at[w]).wait()
        sums = pbuf.at[w, pl.ds(0, (chips - 1) * rows)]
        pltpu.make_async_copy(sums, sums, rs_send.at[w]).wait()
        return carry

    lax.fori_loop(0, nc, drain, 0)
    sent = tabs.at[pl.ds(0, 2 * chips - 1)]
    pltpu.make_async_copy(sent, sent, tab_send).wait()

    @pl.when(c == 0)
    def _():
        for w in range(2):
            push_copy(w).wait_send()


def solution(mesh):
    group_size = mesh.shape['ep']
    chips = group_size // CORES
    hops = chips // 2

    def local_layer(x_loc, idx_loc, gate_loc, w_in, w_out, shared_in, shared_out):
        rows, top_k = idx_loc.shape
        d_model = x_loc.shape[1]
        experts, _, ff = w_in.shape
        fs = shared_in.shape[1]
        num_experts = experts * group_size
        cap = min(rows, LOAD_MULT * rows * top_k // num_experts)
        slots = chips * cap
        nc = d_model // COLS
        any_spec = pl.BlockSpec(memory_space=pl.ANY)
        dma = pltpu.SemaphoreType.DMA
        flops = 2 * group_size * cap * experts * d_model * ff * 2
        return pl.pallas_call(
            functools.partial(moe_kernel, chips, cap, top_k),
            out_shape=pltpu.VMEM((rows, d_model), BF16),
            in_specs=[any_spec] * 7,
            out_specs=pl.BlockSpec(memory_space=pltpu.VMEM),
            scratch_shapes=[
                pltpu.VMEM((nc, group_size * rows, COLS), BF16),
                pltpu.VMEM((top_k, rows), jnp.int32),
                pltpu.VMEM((top_k, rows), F32),
                pltpu.VMEM((group_size, 16, 2 * rows), F32),
                pltpu.VMEM((hops * experts, 2 * rows), F32),
                pltpu.VMEM((2 * experts, chips * rows), F32),
                pltpu.VMEM((2, experts * slots, chips * rows), BF16),
                pltpu.VMEM((2, chips * rows, experts * slots), BF16),
                pltpu.VMEM((experts, slots, PAIR * COLS), BF16),
                pltpu.VMEM((experts, slots, ff), F32),
                pltpu.VMEM((2, experts, slots, ff), BF16),
                pltpu.VMEM((experts * slots, COLS), BF16),
                pltpu.VMEM((nc, chips * rows, COLS), F32),
                pltpu.VMEM((2, chips * rows, COLS), F32),
                pltpu.VMEM((2, nc, hops, rows, COLS), F32),
                pltpu.VMEM((rows, fs), F32),
                pltpu.VMEM((rows, fs), BF16),
                pltpu.VMEM((nc, rows, COLS), F32),
                pltpu.VMEM((2, experts, PAIR * COLS, ff), BF16),
                pltpu.VMEM((WO_SLOTS, experts, ff, COLS), BF16),
                pltpu.VMEM((SI_SLOTS, COLS, fs), BF16),
                pltpu.VMEM((2, fs, COLS), BF16),
                dma((2, nc, hops)), dma((2, hops)), dma((nc,)), dma(()), dma((nc,)), dma(()), dma((3,)),
                dma((2, nc, hops)), dma((nc,)), dma((2,)), dma((nc,)),
                dma((2,)), dma((WO_SLOTS,)), dma((SI_SLOTS,)), dma((2,)),
            ],
            compiler_params=pltpu.CompilerParams(collective_id=0, has_side_effects=True, vmem_limit_bytes=VMEM_BYTES),
            cost_estimate=pl.CostEstimate(flops=flops, bytes_accessed=2 * (w_in.size + w_out.size + shared_in.size + shared_out.size), transcendentals=0),
        )(x_loc, idx_loc.T, gate_loc.T, w_in, w_out, shared_in, shared_out)

    tok_spec = P(('dp', 'ep'), None)
    expert_spec = P('ep', None, None)
    whole_spec = P(None, None)
    return jax.shard_map(local_layer, mesh=mesh, in_specs=(tok_spec, tok_spec, tok_spec, expert_spec, expert_spec, whole_spec, whole_spec), out_specs=tok_spec, check_vma=False)
```
